8 devices in a mesh: dp: 2 (over z, y), sp: 4 (over x, core).
Axes of the slice: x: 2, y: 2, z: 1, core: 2. Of those that a mesh axis runs over, the one named last changes fastest.
Arguments:
- tokens: bfloat16 [256, 2560], P('dp'), parts along dimension 0
- w_query: bfloat16 [2560, 2560], replicated
- w_key: bfloat16 [2560, 256], replicated
- w_value: bfloat16 [2560, 256], replicated
- w_out: bfloat16 [2560, 2560], P('sp')
- k_cache: bfloat16 [256, 2048, 256], P('dp', 'sp'), parts along dimension 0
- v_cache: bfloat16 [256, 2048, 256], P('dp', 'sp'), parts along dimension 0
- positions: int32 [256], P('dp'), parts along dimension 0
Outputs:
- output 1: bfloat16 [256, 2560], P('dp'), parts along dimension 0
- output 2: bfloat16 [256, 2048, 256], P('dp', 'sp'), parts along dimension 0
- output 3: bfloat16 [256, 2048, 256], P('dp', 'sp'), parts along dimension 0
There are 2 independent parts. The reference program is written for one: setup_inputs(seed, part) draws one part's arguments, and reference() takes and returns one part's arrays. A program takes and returns all parts, laid end to end along the dimension named above; an argument that names none is the same for every part.
All inputs are finite; a program needn't handle non-finite values.
Results may differ from the reference program's by a relative error of at most 0.00402993.
Values are sent between devices in bfloat16 or wider.
A program may use at most 1 GiB of HBM per device.

```python
import jax
import jax.numpy as jnp
import math
from jax import lax

BATCH_ROWS = 128
SEQ_LEN = 2048
D_MODEL = 2560
N_HEADS = 10
HEAD_DIM = 256
GAIN_BLOCK = 32


def setup_inputs(seed: int = 0, part: int = 0) -> dict:
    root = jax.random.key(seed)
    shared = jax.random.split(root, 4)
    local = jax.random.split(jax.random.fold_in(root, part), 5)
    q_width = N_HEADS * HEAD_DIM
    align_scale = (math.log(SEQ_LEN) + 0.5) * HEAD_DIM ** -0.5
    tokens = jax.random.normal(local[0], (BATCH_ROWS, D_MODEL), jnp.float32)
    key_raw = jax.random.normal(shared[1], (D_MODEL, HEAD_DIM), jnp.float32)
    w_query = (jax.random.normal(shared[0], (D_MODEL, q_width), jnp.float32) + align_scale * jnp.tile(key_raw, (1, N_HEADS))) * D_MODEL ** -0.5
    w_key = key_raw * D_MODEL ** -0.5
    w_value = jax.random.normal(shared[2], (D_MODEL, HEAD_DIM), jnp.float32) * D_MODEL ** -0.5
    w_out = jax.random.normal(shared[3], (q_width, D_MODEL), jnp.float32) * q_width ** -0.5
    n_blocks = SEQ_LEN // GAIN_BLOCK
    key_gains = jax.random.uniform(local[1], (BATCH_ROWS, n_blocks, 1, 1), jnp.float32, 0.6, 1.6)
    k_cache = (jax.random.normal(local[2], (BATCH_ROWS, n_blocks, GAIN_BLOCK, HEAD_DIM), jnp.float32) * key_gains).reshape(BATCH_ROWS, SEQ_LEN, HEAD_DIM)
    v_cache = jax.random.normal(local[3], (BATCH_ROWS, SEQ_LEN, HEAD_DIM), jnp.float32)
    positions = jax.random.randint(local[4], (BATCH_ROWS,), SEQ_LEN // 4, SEQ_LEN, jnp.int32)
    positions = positions.at[0].set(SEQ_LEN - 1).at[1].set(SEQ_LEN // 4)
    return dict(tokens=tokens.astype(jnp.bfloat16), w_query=w_query.astype(jnp.bfloat16), w_key=w_key.astype(jnp.bfloat16), w_value=w_value.astype(jnp.bfloat16), w_out=w_out.astype(jnp.bfloat16), k_cache=k_cache.astype(jnp.bfloat16), v_cache=v_cache.astype(jnp.bfloat16), positions=positions)


def reference(tokens, w_query, w_key, w_value, w_out, k_cache, v_cache, positions):
    queries = jnp.dot(tokens, w_query, preferred_element_type=jnp.float32).astype(jnp.bfloat16)
    queries = queries.reshape(BATCH_ROWS, N_HEADS, HEAD_DIM)
    key_new = jnp.dot(tokens, w_key, preferred_element_type=jnp.float32).astype(jnp.bfloat16)
    value_new = jnp.dot(tokens, w_value, preferred_element_type=jnp.float32).astype(jnp.bfloat16)
    slot_ids = jnp.arange(SEQ_LEN)
    hit_mask = (slot_ids[None, :] == positions[:, None])[:, :, None]
    k_upd = jnp.where(hit_mask, key_new[:, None, :], k_cache)
    v_upd = jnp.where(hit_mask, value_new[:, None, :], v_cache)

    def one_row(row_args):
        q_row, k_row, v_row, pos_row = row_args
        scores = jnp.dot(q_row, k_row.T, preferred_element_type=jnp.float32) * HEAD_DIM ** -0.5
        scores = jnp.where(slot_ids[None, :] <= pos_row, scores, -jnp.inf)
        weights = jnp.exp(scores - jnp.max(scores, axis=1, keepdims=True))
        weight_sum = jnp.sum(weights, axis=1)
        value_sum = jnp.dot(weights.astype(jnp.bfloat16), v_row, preferred_element_type=jnp.float32)
        return value_sum / weight_sum[:, None]

    head_outs = lax.map(one_row, (queries, k_upd, v_upd, positions))
    attn_heads = head_outs.astype(jnp.bfloat16).reshape(BATCH_ROWS, N_HEADS * HEAD_DIM)
    attn_out = jnp.dot(attn_heads, w_out, preferred_element_type=jnp.float32).astype(jnp.bfloat16)
    return (attn_out, k_upd, v_upd)
```

```python
import functools
import jax
import jax.numpy as jnp
from jax import lax
from jax.sharding import PartitionSpec as P
from jax.experimental import pallas as pl
from jax.experimental.pallas import tpu as pltpu

MESH = pl.DeviceIdType.MESH
F32 = jnp.float32
BF16 = jnp.bfloat16
HEAD_PAD = 16
BLOCK_ROWS = 8
SLOTS = 8
WRITE_LAG = 2
COL_CHUNK = 512


def attention_kernel(n_heads, pos_ref, tok_hbm, wq_hbm, wk_hbm, wv_hbm, wo_hbm, k_hbm, v_hbm,
                     ko_hbm, vo_hbm, o_ref, ml_ref, wo_ref,
                     tok, wq, wk, wv, q_scr, kn_scr, vn_scr, s_scr, w_scr, kbuf, vbuf,
                     wo_sem, w_sems, wq_sems, kin_sems, vin_sems, kout_sems, vout_sems):
    n_rows, seq_local, head_dim = k_hbm.shape
    n_blocks = n_rows // BLOCK_ROWS
    n_slots = kbuf.shape[0]
    base = lax.axis_index('sp') * seq_local
    scale = head_dim ** -0.5

    def reads(blk, slot):
        rows = pl.ds(blk * BLOCK_ROWS, BLOCK_ROWS)
        return (pltpu.make_async_copy(k_hbm.at[rows], kbuf.at[slot], kin_sems.at[slot]),
                pltpu.make_async_copy(v_hbm.at[rows], vbuf.at[slot], vin_sems.at[slot]))

    def writes(blk, slot):
        rows = pl.ds(blk * BLOCK_ROWS, BLOCK_ROWS)
        return (pltpu.make_async_copy(kbuf.at[slot], ko_hbm.at[rows], kout_sems.at[slot]),
                pltpu.make_async_copy(vbuf.at[slot], vo_hbm.at[rows], vout_sems.at[slot]))

    small = [pltpu.make_async_copy(s, d, w_sems.at[i])
             for i, (s, d) in enumerate(((tok_hbm, tok), (wk_hbm, wk), (wv_hbm, wv)))]
    n_chunks = wq.shape[1] // COL_CHUNK
    big = [pltpu.make_async_copy(wq_hbm.at[:, pl.ds(i * COL_CHUNK, COL_CHUNK)],
                                 wq.at[:, pl.ds(i * COL_CHUNK, COL_CHUNK)], wq_sems.at[i])
           for i in range(n_chunks)]
    for c in small + big:
        c.start()
    for s in range(n_slots):
        for c in reads(s, s):
            c.start()
    load_wo = pltpu.make_async_copy(wo_hbm, wo_ref, wo_sem)
    load_wo.start()

    half = head_dim // 2
    for j in range(2):
        q_scr[j, pl.ds(n_heads * n_rows, (HEAD_PAD - n_heads) * n_rows), :] = jnp.zeros(
            ((HEAD_PAD - n_heads) * n_rows, half), F32)
    for c in small:
        c.wait()

    def project(w):
        return jnp.dot(tok[...], w, preferred_element_type=F32).astype(BF16).astype(F32)

    kn_scr[...] = project(wk[...])
    vn_scr[...] = project(wv[...])
    per_chunk = COL_CHUNK // head_dim
    for i in range(n_chunks):
        big[i].wait()
        for h in range(i * per_chunk, (i + 1) * per_chunk):
            q_head = project(wq[:, pl.ds(h * head_dim, head_dim)])
            for j in range(2):
                q_scr[j, pl.ds(h * n_rows, n_rows), :] = q_head[:, j * half:(j + 1) * half]

    lane_t = lax.broadcasted_iota(jnp.int32, (HEAD_PAD, seq_local), 1)
    lane_b = lax.broadcasted_iota(jnp.int32, (HEAD_PAD, n_rows), 1)
    sub16 = lax.broadcasted_iota(jnp.int32, (16, head_dim), 0)

    def block(blk, carry):
        m_acc, l_acc = carry
        slot = lax.rem(blk, n_slots)
        for c in reads(blk, slot):
            c.wait()
        for i in range(BLOCK_ROWS):
            b = blk * BLOCK_ROWS + i
            local = pos_ref[b] - base
            start = pl.multiple_of(jnp.clip(local // 16, 0, seq_local // 16 - 1) * 16, 16)
            for buf, new in ((kbuf, kn_scr), (vbuf, vn_scr)):
                tile = buf[slot, i, pl.ds(start, 16), :].astype(F32)
                row = new[pl.ds(b, 1), :]
                buf[slot, i, pl.ds(start, 16), :] = jnp.where(
                    sub16 == local - start, jnp.broadcast_to(row, (16, head_dim)), tile).astype(BF16)
        for i in range(BLOCK_ROWS):
            b = blk * BLOCK_ROWS + i
            q = jnp.concatenate([q_scr[j, pl.ds(b, HEAD_PAD, stride=n_rows), :] for j in range(2)],
                                axis=1).astype(BF16)
            s_scr[i] = lax.dot_general(q, kbuf[slot, i], (((1,), (1,)), ((), ())),
                                       preferred_element_type=F32)
        for i in range(BLOCK_ROWS):
            b = blk * BLOCK_ROWS + i
            local = pos_ref[b] - base
            s = jnp.where(lane_t <= local, s_scr[i] * scale, -jnp.inf)
            m = jnp.maximum(jnp.max(s, axis=1, keepdims=True), -1e30)
            w = jnp.exp(s - m)
            l = jnp.sum(w, axis=1, keepdims=True)
            w_scr[i] = w.astype(BF16)
            m_acc = jnp.where(lane_b == b, m, m_acc)
            l_acc = jnp.where(lane_b == b, l, l_acc)
        for i in range(BLOCK_ROWS):
            b = blk * BLOCK_ROWS + i
            o = jnp.dot(w_scr[i], vbuf[slot, i], preferred_element_type=F32)
            for j in range(2):
                o_ref[pl.ds(j * n_rows + b, HEAD_PAD, stride=2 * n_rows), :] = o[:, j * half:(j + 1) * half]
        for c in writes(blk, slot):
            c.start()

        @pl.when(jnp.logical_and(blk >= WRITE_LAG, blk - WRITE_LAG + n_slots < n_blocks))
        def _():
            old = blk - WRITE_LAG
            old_slot = lax.rem(old, n_slots)
            for c in writes(old, old_slot):
                c.wait()
            for c in reads(old + n_slots, old_slot):
                c.start()

        return m_acc, l_acc

    zero = jnp.zeros((HEAD_PAD, n_rows), F32)
    load_wo.wait()
    m_acc, l_acc = lax.fori_loop(0, n_blocks, block, (zero, zero))
    ml_ref[pl.ds(0, HEAD_PAD), :] = m_acc
    ml_ref[pl.ds(HEAD_PAD, HEAD_PAD), :] = l_acc
    for blk in range(n_blocks - n_slots, n_blocks):
        for c in writes(blk, blk % n_slots):
            c.wait()


def attention(pos, tok, wq, wk, wv, wo, k, v):
    n_rows, seq_local, head_dim = k.shape
    d_model, q_width = wq.shape
    n_heads = q_width // head_dim
    any_spec = pl.BlockSpec(memory_space=pl.ANY)
    vmem_spec = pl.BlockSpec(memory_space=pltpu.VMEM)
    dma = pltpu.SemaphoreType.DMA
    n_slots = min(SLOTS, n_rows // BLOCK_ROWS)
    return pl.pallas_call(
        functools.partial(attention_kernel, n_heads),
        out_shape=(jax.ShapeDtypeStruct(k.shape, k.dtype), jax.ShapeDtypeStruct(v.shape, v.dtype),
                   pltpu.VMEM((2 * HEAD_PAD * n_rows, head_dim // 2), F32),
                   pltpu.VMEM((2 * HEAD_PAD, n_rows), F32), pltpu.VMEM(wo.shape, BF16)),
        in_specs=[pl.BlockSpec(memory_space=pltpu.SMEM)] + [any_spec] * 7,
        out_specs=(any_spec, any_spec, vmem_spec, vmem_spec, vmem_spec),
        scratch_shapes=[
            pltpu.VMEM(tok.shape, BF16), pltpu.VMEM(wq.shape, BF16),
            pltpu.VMEM(wk.shape, BF16), pltpu.VMEM(wv.shape, BF16),
            pltpu.VMEM((2, HEAD_PAD * n_rows, head_dim // 2), F32),
            pltpu.VMEM((n_rows, head_dim), F32), pltpu.VMEM((n_rows, head_dim), F32),
            pltpu.VMEM((BLOCK_ROWS, HEAD_PAD, seq_local), F32),
            pltpu.VMEM((BLOCK_ROWS, HEAD_PAD, seq_local), BF16),
            pltpu.VMEM((n_slots, BLOCK_ROWS, seq_local, head_dim), BF16),
            pltpu.VMEM((n_slots, BLOCK_ROWS, seq_local, head_dim), BF16),
            dma, dma((3,)), dma((q_width // COL_CHUNK,)),
            dma((n_slots,)), dma((n_slots,)), dma((n_slots,)), dma((n_slots,))],
        compiler_params=pltpu.CompilerParams(vmem_limit_bytes=54 * 1024 * 1024),
        cost_estimate=pl.CostEstimate(flops=10**10, bytes_accessed=150 * 10**6, transcendentals=0),
        name='attention',
    )(pos, tok, wq, wk, wv, wo, k, v)


def combine_kernel(o_ref, ml_ref, wo, y_ref,
                   po, pml, oc, mlc, om, xo, xml, fbuf, ob, yq, yp, ym, yx, yxr, yb, yg,
                   send, recv):
    n_rows = y_ref.shape[0]
    rows_local, d_model = wo.shape
    units = rows_local // 128
    span = units * n_rows
    quarter = d_model // 4
    me = lax.axis_index('sp')
    core = lax.rem(me, 2)
    chip = me // 2
    partner = chip * 2 + 1 - core
    cross = (1 - chip) * 2 + core

    barrier = pltpu.get_barrier_semaphore()
    for peer in (partner, cross):
        pl.semaphore_signal(barrier, inc=1, device_id={'sp': peer}, device_id_type=MESH)
    pl.semaphore_wait(barrier, 2)

    def remote(i, src, dst, peer):
        return pltpu.make_async_remote_copy(src_ref=src, dst_ref=dst, send_sem=send.at[i], recv_sem=recv.at[i],
                                            device_id={'sp': peer}, device_id_type=MESH)

    def part(dest):
        return o_ref.at[pl.ds(pl.multiple_of(dest * span, span), span)]

    far, near = (1 - chip) * 2, chip * 2
    p_ml = remote(0, ml_ref, pml, partner)
    p_far = remote(1, part(far + 1 - core), po.at[0], partner)
    p_near = remote(2, part(near + 1 - core), po.at[1], partner)
    for c in (p_ml, p_far, p_near):
        c.start()

    def merge(a, b):
        peak = jnp.maximum(a[:HEAD_PAD], b[:HEAD_PAD])
        fa = jnp.exp(a[:HEAD_PAD] - peak)
        fb = jnp.exp(b[:HEAD_PAD] - peak)
        return fa, fb, peak, a[HEAD_PAD:] * fa + b[HEAD_PAD:] * fb

    def columns(k, dest):
        picks = [fbuf[k, pl.ds((dest * units + u) // 2, 1), :] for u in range(units)]
        picks += [picks[-1]] * (8 - units)
        return jnp.concatenate(picks, axis=0).T

    p_ml.wait_recv()
    fa, fb, peak, total = merge(ml_ref[...], pml[...])
    fbuf[0] = fa
    fbuf[1] = fb
    mlc[pl.ds(0, HEAD_PAD), :] = peak
    mlc[pl.ds(HEAD_PAD, HEAD_PAD), :] = total
    x_ml = remote(3, mlc, xml, cross)
    x_ml.start()

    def chip_part(dest, slot, dst):
        ca, cb = columns(0, dest), columns(1, dest)
        for u in range(units):
            mine = o_ref[pl.ds(pl.multiple_of(dest * span + u * n_rows, n_rows), n_rows), :]
            theirs = po[slot, pl.ds(u * n_rows, n_rows), :]
            dst[pl.ds(u * n_rows, n_rows), :] = mine * ca[:, u:u + 1] + theirs * cb[:, u:u + 1]

    p_far.wait_recv()
    chip_part(far + core, 0, oc)
    x_o = remote(4, oc, xo, cross)
    x_o.start()
    p_near.wait_recv()
    chip_part(me, 1, om)

    x_ml.wait_recv()
    fa, fb, peak, total = merge(mlc[...], xml[...])
    fbuf[2] = fa
    fbuf[3] = fb
    fbuf[4] = total
    ca, cb, cl = columns(2, me), columns(3, me), columns(4, me)
    x_o.wait_recv()
    for u in range(units):
        rows = pl.ds(u * n_rows, n_rows)
        value = om[rows, :] * ca[:, u:u + 1] + xo[rows, :] * cb[:, u:u + 1]
        ob[:, u * 128:(u + 1) * 128] = (value / cl[:, u:u + 1]).astype(BF16)

    def product(c, x):
        cols = pl.ds(pl.multiple_of((c * 2 + x) * quarter, quarter), quarter)
        return jnp.dot(ob[...], wo[:, cols], preferred_element_type=F32)

    yq[0] = product(1 - core, 1 - chip)
    p_y0 = remote(5, yq.at[0], yp.at[0], partner)
    p_y0.start()
    yq[1] = product(1 - core, chip)
    p_y1 = remote(6, yq.at[1], yp.at[1], partner)
    p_y1.start()
    ym[...] = product(core, 1 - chip)
    p_y0.wait_recv()
    yx[...] = ym[...] + yp[0]
    x_y = remote(7, yx, yxr, cross)
    x_y.start()
    ym[...] = product(core, chip)
    p_y1.wait_recv()
    ym[...] = ym[...] + yp[1]
    x_y.wait_recv()
    yb[...] = (ym[...] + yxr[...]).astype(BF16)
    x_b = remote(8, yb, yg.at[0], cross)
    p_b = remote(9, yb, yg.at[1], partner)
    x_b.start()
    p_b.start()
    x_b.wait_recv()
    p_f = remote(10, yg.at[0], yg.at[2], partner)
    p_f.start()

    def place(c, x, value):
        y_ref[:, pl.ds(pl.multiple_of((c * 2 + x) * quarter, quarter), quarter)] = value

    place(core, chip, yb[...])
    place(core, 1 - chip, yg[0])
    p_b.wait_recv()
    place(1 - core, chip, yg[1])
    p_f.wait_recv()
    place(1 - core, 1 - chip, yg[2])
    for c in (p_ml, p_far, p_near, x_ml, x_o, p_y0, p_y1, x_y, x_b, p_b, p_f):
        c.wait_send()


def combine(o, ml, w_out, n_rows):
    rows_local, d_model = w_out.shape
    units = rows_local // 128
    span = units * n_rows
    quarter = d_model // 4
    vmem = pl.BlockSpec(memory_space=pltpu.VMEM)
    part = pltpu.VMEM((span, 128), F32)
    tail = pltpu.VMEM((n_rows, quarter), F32)
    return pl.pallas_call(
        combine_kernel,
        out_shape=jax.ShapeDtypeStruct((n_rows, d_model), BF16),
        in_specs=[vmem, vmem, vmem],
        out_specs=vmem,
        scratch_shapes=[
            pltpu.VMEM((2, span, 128), F32), pltpu.VMEM(ml.shape, F32),
            part, pltpu.VMEM(ml.shape, F32), part, part, pltpu.VMEM(ml.shape, F32),
            pltpu.VMEM((5, HEAD_PAD, n_rows), F32), pltpu.VMEM((n_rows, rows_local), BF16),
            pltpu.VMEM((2, n_rows, quarter), F32), pltpu.VMEM((2, n_rows, quarter), F32),
            tail, tail, tail, pltpu.VMEM((n_rows, quarter), BF16), pltpu.VMEM((3, n_rows, quarter), BF16),
            pltpu.SemaphoreType.DMA((11,)), pltpu.SemaphoreType.DMA((11,))],
        compiler_params=pltpu.CompilerParams(collective_id=0, has_side_effects=True,
                                             vmem_limit_bytes=40 * 1024 * 1024),
        name='combine',
    )(o, ml, w_out)


def solution(mesh):
    def local_step(tokens, w_query, w_key, w_value, w_out, k_cache, v_cache, positions):
        k_upd, v_upd, o, ml, wo = attention(positions, tokens, w_query, w_key, w_value, w_out, k_cache, v_cache)
        attn_out = combine(o, ml, wo, k_cache.shape[0])
        return attn_out, k_upd, v_upd

    cache_spec = P('dp', 'sp', None)
    return jax.shard_map(local_step, mesh=mesh, in_specs=(P('dp', None), P(), P(), P(), P('sp', None), cache_spec, cache_spec, P('dp')), out_specs=(P('dp', None), cache_spec, cache_spec), check_vma=False)
```

```python
import functools
import jax
import jax.numpy as jnp
from jax import lax
from jax.sharding import PartitionSpec as P
from jax.experimental import pallas as pl
from jax.experimental.pallas import tpu as pltpu

MESH = pl.DeviceIdType.MESH
F32 = jnp.float32
BF16 = jnp.bfloat16
HEAD_PAD = 16
BLOCK_ROWS = 8
COL_CHUNK = 512
PIECES = (16,) * 4
FIRST_ROWS = 128 - sum(PIECES)
GROUPS = (FIRST_ROWS, 32, 16, 16)
KINDS = ('quarter', 'quarter', 'quarter', 'half')
READ_AHEAD = 4
MIB = 1024 * 1024
ANY_SPEC = pl.BlockSpec(memory_space=pl.ANY)
VMEM_SPEC = pl.BlockSpec(memory_space=pltpu.VMEM)
SMEM_SPEC = pl.BlockSpec(memory_space=pltpu.SMEM)
DMA = pltpu.SemaphoreType.DMA


def patch_rows(buf, new, first, pos_ref, base, rows):
    seq_local, head_dim = buf.shape[-2:]
    sub = lax.broadcasted_iota(jnp.int32, (16, head_dim), 0)
    for i in rows:
        local = pos_ref[first + i] - base
        start = pl.multiple_of(jnp.clip(local // 16, 0, seq_local // 16 - 1) * 16, 16)
        tile = buf[i, pl.ds(start, 16), :].astype(F32)
        row = jnp.broadcast_to(new[pl.ds(first + i, 1), :], (16, head_dim))
        buf[i, pl.ds(start, 16), :] = jnp.where(sub == local - start, row, tile).astype(BF16)


def attend(first, pos_ref, base, scale, q_ref, kb, vb, s_scr, w_scr, o_ref, lane0, o_rows, carry, new=None):
    seq_local, head_dim = kb.shape[-2:]
    n_all = q_ref.shape[1] // HEAD_PAD
    half = head_dim // 2
    lane_t = lax.broadcasted_iota(jnp.int32, (HEAD_PAD, seq_local), 1)
    lane_b = lax.broadcasted_iota(jnp.int32, (HEAD_PAD, 128), 1)
    m_acc, l_acc = carry

    def query(b):
        return jnp.concatenate([q_ref[j, pl.ds(b, HEAD_PAD, stride=n_all), :] for j in range(2)], axis=1)

    for i in range(BLOCK_ROWS):
        s_scr[i] = lax.dot_general(query(first + i).astype(BF16), kb[i], (((1,), (1,)), ((), ())),
                                   preferred_element_type=F32)
    extra = []
    for i in range(BLOCK_ROWS):
        b = first + i
        local = pos_ref[b] - base
        s = s_scr[i]
        if new is not None:
            s_new = jnp.sum(query(b) * new[0][pl.ds(b, 1), :], axis=1, keepdims=True)
            s = jnp.where(lane_t == local, s_new, s)
        s = jnp.where(lane_t <= local, s * scale, -jnp.inf)
        m = jnp.maximum(jnp.max(s, axis=1, keepdims=True), -1e30)
        w = jnp.exp(s - m)
        l = jnp.sum(w, axis=1, keepdims=True)
        if new is not None:
            hit = lane_t == local
            extra.append(jnp.sum(jnp.where(hit, w, 0.0), axis=1, keepdims=True))
            w = jnp.where(hit, 0.0, w)
        w_scr[i] = w.astype(BF16)
        m_acc = jnp.where(lane_b == lane0 + i, m, m_acc)
        l_acc = jnp.where(lane_b == lane0 + i, l, l_acc)
    for i in range(BLOCK_ROWS):
        o = jnp.dot(w_scr[i], vb[i], preferred_element_type=F32)
        if new is not None:
            o = o + extra[i].astype(BF16).astype(F32) * new[1][pl.ds(first + i, 1), :]
        for j in range(2):
            o_ref[pl.ds(j * o_rows + lane0 + i, HEAD_PAD, stride=2 * o_rows), :] = o[:, j * half:(j + 1) * half]
    return m_acc, l_acc


def store_ml(ml_ref, carry):
    ml_ref[pl.ds(0, HEAD_PAD), :] = carry[0]
    ml_ref[pl.ds(HEAD_PAD, HEAD_PAD), :] = carry[1]


def zero_carry():
    return jnp.zeros((HEAD_PAD, 128), F32), jnp.zeros((HEAD_PAD, 128), F32)


def first_kernel(n_heads, pos_ref, tok_hbm, wq_hbm, wk_hbm, wv_hbm, k_hbm, v_hbm,
                 ko_hbm, vo_hbm, q_ref, kn_ref, vn_ref, o_ref, ml_ref,
                 tok, wq, wk, wv, s_scr, w_scr, kbuf, vbuf,
                 w_sems, wq_sems, kin_sems, vin_sems, kout_sems, vout_sems):
    n_rows, seq_local, head_dim = k_hbm.shape
    n_blocks = kbuf.shape[0]
    base = lax.axis_index('sp') * seq_local
    half = head_dim // 2

    def reads(blk):
        rows = pl.ds(blk * BLOCK_ROWS, BLOCK_ROWS)
        return (pltpu.make_async_copy(k_hbm.at[rows], kbuf.at[blk], kin_sems.at[blk]),
                pltpu.make_async_copy(v_hbm.at[rows], vbuf.at[blk], vin_sems.at[blk]))

    def writes(blk):
        rows = pl.ds(blk * BLOCK_ROWS, BLOCK_ROWS)
        return (pltpu.make_async_copy(kbuf.at[blk], ko_hbm.at[rows], kout_sems.at[blk]),
                pltpu.make_async_copy(vbuf.at[blk], vo_hbm.at[rows], vout_sems.at[blk]))

    small = [pltpu.make_async_copy(s, d, w_sems.at[i])
             for i, (s, d) in enumerate(((tok_hbm, tok), (wk_hbm, wk), (wv_hbm, wv)))]
    n_chunks = wq.shape[1] // COL_CHUNK
    big = [pltpu.make_async_copy(wq_hbm.at[:, pl.ds(i * COL_CHUNK, COL_CHUNK)],
                                 wq.at[:, pl.ds(i * COL_CHUNK, COL_CHUNK)], wq_sems.at[i])
           for i in range(n_chunks)]
    for c in small + big:
        c.start()
    for c in reads(0):
        c.start()
    for j in range(2):
        q_ref[j, pl.ds(n_heads * n_rows, (HEAD_PAD - n_heads) * n_rows), :] = jnp.zeros(
            ((HEAD_PAD - n_heads) * n_rows, half), F32)
    for c in small:
        c.wait()

    def project(w):
        return jnp.dot(tok[...], w, preferred_element_type=F32).astype(BF16).astype(F32)

    kn_ref[...] = project(wk[...])
    vn_ref[...] = project(wv[...])
    per_chunk = COL_CHUNK // head_dim

    def pass_through(blk):
        for c in reads(blk):
            c.wait()
        patch_rows(kbuf.at[blk], kn_ref, blk * BLOCK_ROWS, pos_ref, base, range(BLOCK_ROWS))
        patch_rows(vbuf.at[blk], vn_ref, blk * BLOCK_ROWS, pos_ref, base, range(BLOCK_ROWS))
        for c in writes(blk):
            c.start()

    for i in range(n_chunks):
        if i + 1 < n_blocks:
            for c in reads(i + 1):
                c.start()
        big[i].wait()
        for h in range(i * per_chunk, (i + 1) * per_chunk):
            q_head = project(wq[:, pl.ds(h * head_dim, head_dim)])
            for j in range(2):
                q_ref[j, pl.ds(h * n_rows, n_rows), :] = q_head[:, j * half:(j + 1) * half]
    for blk in range(n_chunks + 1, n_blocks):
        for c in reads(blk):
            c.start()

    def block(blk, carry):
        pass_through(blk)
        return attend(blk * BLOCK_ROWS, pos_ref, base, head_dim ** -0.5, q_ref, kbuf.at[blk], vbuf.at[blk],
                      s_scr, w_scr, o_ref, blk * BLOCK_ROWS, n_blocks * BLOCK_ROWS, carry)

    store_ml(ml_ref, lax.fori_loop(0, n_blocks, block, zero_carry()))
    for blk in range(n_blocks):
        for c in writes(blk):
            c.wait()


def first_part(pos, tok, wq, wk, wv, k, v):
    n_rows, seq_local, head_dim = k.shape
    d_model, q_width = wq.shape
    n_heads = q_width // head_dim
    n_blocks = FIRST_ROWS // BLOCK_ROWS
    block = pltpu.VMEM((n_blocks, BLOCK_ROWS, seq_local, head_dim), BF16)
    return pl.pallas_call(
        functools.partial(first_kernel, n_heads),
        out_shape=(jax.ShapeDtypeStruct(k.shape, k.dtype), jax.ShapeDtypeStruct(v.shape, v.dtype),
                   pltpu.VMEM((2, HEAD_PAD * n_rows, head_dim // 2), F32),
                   pltpu.VMEM((n_rows, head_dim), F32), pltpu.VMEM((n_rows, head_dim), F32),
                   pltpu.VMEM((2 * HEAD_PAD * FIRST_ROWS, head_dim // 2), F32),
                   pltpu.VMEM((2 * HEAD_PAD, 128), F32)),
        in_specs=[SMEM_SPEC] + [ANY_SPEC] * 6,
        out_specs=(ANY_SPEC, ANY_SPEC) + (VMEM_SPEC,) * 5,
        scratch_shapes=[
            pltpu.VMEM(tok.shape, BF16), pltpu.VMEM(wq.shape, BF16),
            pltpu.VMEM(wk.shape, BF16), pltpu.VMEM(wv.shape, BF16),
            pltpu.VMEM((BLOCK_ROWS, HEAD_PAD, seq_local), F32),
            pltpu.VMEM((BLOCK_ROWS, HEAD_PAD, seq_local), BF16),
            block, block,
            DMA((3,)), DMA((q_width // COL_CHUNK,)),
            DMA((n_blocks,)), DMA((n_blocks,)), DMA((n_blocks,)), DMA((n_blocks,))],
        compiler_params=pltpu.CompilerParams(vmem_limit_bytes=60 * MIB),
        cost_estimate=pl.CostEstimate(flops=10**10, bytes_accessed=70 * 10**6, transcendentals=0),
        name='attention_first',
    )(pos, tok, wq, wk, wv, k, v)


COPIES = 10
N_PIECES = len(PIECES)
PIECE_ROW0 = tuple(sum(PIECES[:i]) for i in range(N_PIECES))


class Group:
    def __init__(self):
        self.copies = {}

    def __getattr__(self, name):
        return self.__dict__['copies'][name]()


def rest_kernel(pos_ref, q_ref, kn_ref, vn_ref, o0, ml0, wo_hbm, k_hbm, v_hbm,
                *refs):
    kret, vret = refs[:N_PIECES], refs[N_PIECES:2 * N_PIECES]
    rest_body(pos_ref, q_ref, kn_ref, vn_ref, o0, ml0, wo_hbm, k_hbm, v_hbm, kret, vret, *refs[2 * N_PIECES:])


def rest_body(pos_ref, q_ref, kn_ref, vn_ref, o0, ml0, wo_hbm, k_hbm, v_hbm,
              kret, vret, y_ref, wo, s_scr, w_scr, fbuf, wo_sem, kin_sems, vin_sems, send, recv, *scratch):
    n_rows, seq_local, head_dim = k_hbm.shape
    rows_local, d_model = wo.shape
    units = rows_local // 128
    half_width = d_model // 2
    n_blocks = sum(PIECES) // BLOCK_ROWS
    me = lax.axis_index('sp')
    base = me * seq_local
    core = lax.rem(me, 2)
    chip = me // 2
    partner = chip * 2 + 1 - core
    cross = (1 - chip) * 2 + core
    far, near = (1 - chip) * 2, chip * 2

    def reads(blk):
        p = piece_of(blk)
        src = pl.ds(FIRST_ROWS + blk * BLOCK_ROWS, BLOCK_ROWS)
        dst = pl.ds(blk * BLOCK_ROWS - PIECE_ROW0[p], BLOCK_ROWS)
        return (pltpu.make_async_copy(k_hbm.at[src], kret[p].at[dst], kin_sems.at[blk]),
                pltpu.make_async_copy(v_hbm.at[src], vret[p].at[dst], vin_sems.at[blk]))

    barrier = pltpu.get_barrier_semaphore()
    for peer in (partner, cross):
        pl.semaphore_signal(barrier, inc=1, device_id={'sp': peer}, device_id_type=MESH)
    for blk in range(min(READ_AHEAD, n_blocks)):
        for c in reads(blk):
            c.start()
    load_wo = pltpu.make_async_copy(wo_hbm, wo, wo_sem)
    load_wo.start()

    def group(idx):
        g = Group()
        g.n, g.row0 = GROUPS[idx], sum(GROUPS[:idx])
        refs = scratch[idx * len(BUFS):(idx + 1) * len(BUFS)]
        for name, ref in zip(BUFS, refs):
            setattr(g, name, ref)
        if idx == 0:
            g.o, g.ml = o0, ml0
        g.span = units * g.n

        def remote(i, src, dst, peer):
            return pltpu.make_async_remote_copy(src_ref=src, dst_ref=dst, send_sem=send.at[idx, i],
                                                recv_sem=recv.at[idx, i], device_id={'sp': peer},
                                                device_id_type=MESH)

        def part(dest):
            return g.o.at[pl.ds(pl.multiple_of(dest * g.span, 8), g.span)]

        g.copies['p_ml'] = lambda: remote(0, g.ml, g.pml, partner)
        g.copies['p_far'] = lambda: remote(1, part(far + 1 - core), g.po.at[0], partner)
        g.copies['p_near'] = lambda: remote(2, part(near + 1 - core), g.po.at[1], partner)
        g.copies['x_ml'] = lambda: remote(3, g.mlc, g.xml, cross)
        g.copies['x_o'] = lambda: remote(4, g.oc, g.xo, cross)
        g.copies['p_y'] = lambda: remote(5, g.yq, g.yp, partner)
        g.copies['x_y'] = lambda: remote(6, g.yx, g.yxr, cross)
        if KINDS[idx] == 'half':
            g.copies['p_b'] = lambda: remote(7, g.yb, g.yg, partner)
        else:
            g.copies['p_b'] = lambda: remote(7, g.yb, g.yg.at[1], partner)
            g.copies['x_b'] = lambda: remote(8, g.yb, g.yg.at[0], cross)
            g.copies['p_f'] = lambda: remote(9, g.yg.at[0], g.yg.at[2], partner)
        return g

    def merge(a, b):
        peak = jnp.maximum(a[:HEAD_PAD], b[:HEAD_PAD])
        fa = jnp.exp(a[:HEAD_PAD] - peak)
        fb = jnp.exp(b[:HEAD_PAD] - peak)
        return fa, fb, peak, a[HEAD_PAD:] * fa + b[HEAD_PAD:] * fb

    def columns(k, dest, n):
        picks = [fbuf[k, pl.ds((dest * units + u) // 2, 1), :] for u in range(units)]
        picks += [picks[-1]] * (8 - units)
        return jnp.concatenate(picks, axis=0).T[:n]

    def stage0(g):
        for c in (g.p_ml, g.p_far, g.p_near):
            c.start()

    def stage1(g):
        g.p_ml.wait_recv()
        fa, fb, peak, total = merge(g.ml[...], g.pml[...])
        fbuf[0] = fa
        fbuf[1] = fb
        g.mlc[pl.ds(0, HEAD_PAD), :] = peak
        g.mlc[pl.ds(HEAD_PAD, HEAD_PAD), :] = total
        g.x_ml.start()

        def chip_part(dest, slot, dst):
            ca, cb = columns(0, dest, g.n), columns(1, dest, g.n)
            for u in range(units):
                mine = g.o[pl.ds(pl.multiple_of(dest * g.span + u * g.n, 8), g.n), :]
                theirs = g.po[slot, pl.ds(u * g.n, g.n), :]
                dst[pl.ds(u * g.n, g.n), :] = mine * ca[:, u:u + 1] + theirs * cb[:, u:u + 1]

        g.p_far.wait_recv()
        chip_part(far + core, 0, g.oc)
        g.x_o.start()
        g.p_near.wait_recv()
        chip_part(me, 1, g.om)

    def stage2(g):
        g.x_ml.wait_recv()
        fa, fb, peak, total = merge(g.mlc[...], g.xml[...])
        fbuf[2] = fa
        fbuf[3] = fb
        fbuf[4] = total
        ca, cb, cl = columns(2, me, g.n), columns(3, me, g.n), columns(4, me, g.n)
        g.x_o.wait_recv()
        for u in range(units):
            rows = pl.ds(u * g.n, g.n)
            value = g.om[rows, :] * ca[:, u:u + 1] + g.xo[rows, :] * cb[:, u:u + 1]
            g.ob[:, u * 128:(u + 1) * 128] = (value / cl[:, u:u + 1]).astype(BF16)

        def product(c):
            cols = pl.ds(pl.multiple_of(c * half_width, 128), half_width)
            return jnp.dot(g.ob[...], wo[:, cols], preferred_element_type=F32)

        g.yq[...] = product(1 - core)
        g.p_y.start()
        g.ym[...] = product(core)

    def place(g, start, value):
        width = value.shape[1]
        y_ref[pl.ds(g.row0, g.n), pl.ds(pl.multiple_of(start, 128), width)] = value

    def stage3_half(g):
        g.p_y.wait_recv()
        g.yx[...] = g.ym[...] + g.yp[...]
        g.x_y.start()

    def stage4_half(g):
        g.x_y.wait_recv()
        g.yb[...] = (g.yx[...] + g.yxr[...]).astype(BF16)
        g.p_b.start()
        place(g, core * half_width, g.yb[...])

    def finish(g):
        for name in g.copies:
            g.copies[name]().wait_send()

    def stage5_half(g):
        g.p_b.wait_recv()
        place(g, (1 - core) * half_width, g.yg[...])
        finish(g)

    quarter = half_width // 2
    far_cols = pl.ds(pl.multiple_of((1 - chip) * quarter, 128), quarter)
    near_cols = pl.ds(pl.multiple_of(chip * quarter, 128), quarter)

    def stage3_quarter(g):
        g.p_y.wait_recv()
        g.yx[...] = g.ym[:, far_cols] + g.yp[:, far_cols]
        g.x_y.start()
        g.yn[...] = g.ym[:, near_cols] + g.yp[:, near_cols]

    def stage4_quarter(g):
        g.x_y.wait_recv()
        g.yb[...] = (g.yn[...] + g.yxr[...]).astype(BF16)
        g.x_b.start()
        g.p_b.start()
        place(g, core * half_width + chip * quarter, g.yb[...])

    def stage5_quarter(g):
        g.x_b.wait_recv()
        g.p_f.start()
        place(g, core * half_width + (1 - chip) * quarter, g.yg[0])

    def stage6_quarter(g):
        g.p_b.wait_recv()
        place(g, (1 - core) * half_width + chip * quarter, g.yg[1])
        g.p_f.wait_recv()
        place(g, (1 - core) * half_width + (1 - chip) * quarter, g.yg[2])
        finish(g)

    common = (stage0, stage1, stage2)
    stages = dict(half=common + (stage3_half, stage4_half, stage5_half),
                  quarter=common + (stage3_quarter, stage4_quarter, stage5_quarter, stage6_quarter))
    groups = [group(i) for i in range(len(GROUPS))]

    def attend_block(blk):
        if blk + READ_AHEAD < n_blocks:
            for c in reads(blk + READ_AHEAD):
                c.start()
        for c in reads(blk):
            c.wait()
        p = piece_of(blk)
        row = FIRST_ROWS + blk * BLOCK_ROWS
        idx = [i for i in range(len(GROUPS)) if row >= sum(GROUPS[:i])][-1]
        g = groups[idx]
        lane0 = row - g.row0
        carry = zero_carry() if lane0 == 0 else (g.ml[pl.ds(0, HEAD_PAD), :], g.ml[pl.ds(HEAD_PAD, HEAD_PAD), :])
        rows = pl.ds(blk * BLOCK_ROWS - PIECE_ROW0[p], BLOCK_ROWS)
        store_ml(g.ml, attend(row, pos_ref, base, head_dim ** -0.5, q_ref, kret[p].at[rows], vret[p].at[rows],
                              s_scr, w_scr, g.o, lane0, g.n, carry, (kn_ref, vn_ref)))

    for action in SCHEDULE:
        if isinstance(action, int):
            attend_block(action)
        elif action == 'wo':
            load_wo.wait()
        elif action == 'barrier':
            pl.semaphore_wait(barrier, 2)
        else:
            stages[KINDS[action[0]]][action[1]](groups[action[0]])


def piece_of(blk):
    return [i for i in range(N_PIECES) if blk * BLOCK_ROWS >= PIECE_ROW0[i]][-1]


BUFS = ('o', 'ml', 'pml', 'po', 'mlc', 'oc', 'om', 'xo', 'xml', 'ob', 'yq', 'yp', 'ym', 'yn', 'yx', 'yxr', 'yb',
        'yg')
SCHEDULE = ('barrier', (0, 0), 0, (0, 1), 1, 2, 3, (1, 0), 4, (1, 1), 5, (2, 0), 'wo', (0, 2), (2, 1), 6, (0,
            3), 7, (3, 0), (1, 2), (3, 1), (2, 2), (1, 3), (2, 3), (0, 4), (3, 2), (1, 4), (3, 3), (2, 4), (0,
            5), (1, 5), (0, 6), (1, 6), (3, 4), (2, 5), (3, 5), (2, 6))


def rest_part(pos, q, kn, vn, o0, ml0, wo, k, v):
    n_rows, seq_local, head_dim = k.shape
    rows_local, d_model = wo.shape
    units = rows_local // 128
    n_blocks = sum(PIECES) // BLOCK_ROWS

    def buffers(n, own, kind):
        span = units * n
        ml, part, half = (2 * HEAD_PAD, 128), (span, 128), (n, d_model // 2)
        slab = half if kind == 'half' else (n, d_model // 4)
        shapes = dict(o=((2 * HEAD_PAD * n if own else 8, 128), F32), ml=(ml, F32),
                      pml=(ml, F32), po=((2,) + part, F32), mlc=(ml, F32), oc=(part, F32), om=(part, F32),
                      xo=(part, F32), xml=(ml, F32), ob=((n, rows_local), BF16), yq=(half, F32), yp=(half, F32),
                      ym=(half, F32), yn=(slab if kind != 'half' else (8, 128), F32), yx=(slab, F32),
                      yxr=(slab, F32), yb=(slab, BF16), yg=(slab if kind == 'half' else (3,) + slab, BF16))
        return [pltpu.VMEM(*shapes[name]) for name in BUFS]

    return pl.pallas_call(
        rest_kernel,
        out_shape=tuple(pltpu.VMEM((n, seq_local, head_dim), BF16) for n in PIECES * 2)
        + (pltpu.VMEM((n_rows, d_model), BF16),),
        in_specs=[SMEM_SPEC] + [VMEM_SPEC] * 5 + [ANY_SPEC] * 3,
        out_specs=(VMEM_SPEC,) * (2 * N_PIECES + 1),
        scratch_shapes=[
            pltpu.VMEM(wo.shape, BF16),
            pltpu.VMEM((BLOCK_ROWS, HEAD_PAD, seq_local), F32),
            pltpu.VMEM((BLOCK_ROWS, HEAD_PAD, seq_local), BF16),
            pltpu.VMEM((5, HEAD_PAD, 128), F32),
            DMA, DMA((n_blocks,)), DMA((n_blocks,)), DMA((len(GROUPS), COPIES)), DMA((len(GROUPS), COPIES))]
            + [b for i, n in enumerate(GROUPS) for b in buffers(n, i > 0, KINDS[i])],
        compiler_params=pltpu.CompilerParams(collective_id=0, has_side_effects=True, vmem_limit_bytes=REST_VMEM * MIB),
        cost_estimate=pl.CostEstimate(flops=10**10, bytes_accessed=40 * 10**6, transcendentals=0),
        name='attention_rest',
    )(pos, q, kn, vn, o0, ml0, wo, k, v)


REST_VMEM = 18


def write_kernel(pos_ref, kn_ref, vn_ref, y_ref, *refs):
    ko_hbm, vo_hbm, y_hbm = refs[2 * N_PIECES + 2:2 * N_PIECES + 5]
    kret, vret = refs[2 * N_PIECES + 5:3 * N_PIECES + 5], refs[3 * N_PIECES + 5:4 * N_PIECES + 5]
    k_sems, v_sems, y_sem = refs[4 * N_PIECES + 5:]
    seq_local = ko_hbm.shape[1]
    n_blocks = sum(PIECES) // BLOCK_ROWS
    base = lax.axis_index('sp') * seq_local
    write_y = pltpu.make_async_copy(y_ref, y_hbm, y_sem)

    def writes(blk):
        p = piece_of(blk)
        src = pl.ds(blk * BLOCK_ROWS - PIECE_ROW0[p], BLOCK_ROWS)
        dst = pl.ds(FIRST_ROWS + blk * BLOCK_ROWS, BLOCK_ROWS)
        return (pltpu.make_async_copy(kret[p].at[src], ko_hbm.at[dst], k_sems.at[blk]),
                pltpu.make_async_copy(vret[p].at[src], vo_hbm.at[dst], v_sems.at[blk]))

    for blk in range(n_blocks):
        p = piece_of(blk)
        rows = pl.ds(blk * BLOCK_ROWS - PIECE_ROW0[p], BLOCK_ROWS)
        for kept, new, copy in zip((kret, vret), (kn_ref, vn_ref), writes(blk)):
            patch_rows(kept[p].at[rows], new, FIRST_ROWS + blk * BLOCK_ROWS, pos_ref, base, range(BLOCK_ROWS))
            copy.start()
    write_y.start()
    write_y.wait()
    for blk in range(n_blocks):
        for c in writes(blk):
            c.wait()


def write_part(pos, kn, vn, y, ko, vo, kret, vret):
    n_blocks = sum(PIECES) // BLOCK_ROWS
    kept = (*kret, *vret)
    out = pl.pallas_call(
        write_kernel,
        out_shape=(jax.ShapeDtypeStruct(ko.shape, ko.dtype), jax.ShapeDtypeStruct(vo.shape, vo.dtype),
                   jax.ShapeDtypeStruct(y.shape, y.dtype)) + tuple(pltpu.VMEM(a.shape, a.dtype) for a in kept),
        in_specs=[SMEM_SPEC, VMEM_SPEC, VMEM_SPEC, VMEM_SPEC] + [VMEM_SPEC] * (2 * N_PIECES) + [ANY_SPEC, ANY_SPEC],
        out_specs=(ANY_SPEC, ANY_SPEC, ANY_SPEC) + (VMEM_SPEC,) * (2 * N_PIECES),
        input_output_aliases={4 + 2 * N_PIECES: 0, 5 + 2 * N_PIECES: 1,
                              **{4 + i: 3 + i for i in range(2 * N_PIECES)}},
        scratch_shapes=[DMA((n_blocks,)), DMA((n_blocks,)), DMA],
        compiler_params=pltpu.CompilerParams(vmem_limit_bytes=REST_VMEM * MIB),
        cost_estimate=pl.CostEstimate(flops=10**10, bytes_accessed=40 * 10**6, transcendentals=0),
        name='attention_write',
    )(pos, kn, vn, y, *kept, ko, vo)
    return out[2], out[0], out[1]


def in_vmem(*arrays):
    return [pltpu.with_memory_space_constraint(a, pltpu.VMEM) for a in arrays]


def solution(mesh):
    def local_step(tokens, w_query, w_key, w_value, w_out, k_cache, v_cache, positions):
        ko, vo, q, kn, vn, o0, ml0 = first_part(
            positions, tokens, w_query, w_key, w_value, k_cache, v_cache)
        q, kn, vn, o0, ml0 = in_vmem(q, kn, vn, o0, ml0)
        *kept, y = rest_part(positions, q, kn, vn, o0, ml0, w_out, k_cache, v_cache)
        *kept, y = in_vmem(*kept, y)
        return write_part(positions, kn, vn, y, ko, vo, kept[:N_PIECES], kept[N_PIECES:])

    cache_spec = P('dp', 'sp', None)
    return jax.shard_map(local_step, mesh=mesh, in_specs=(P('dp', None), P(), P(), P(), P('sp', None), cache_spec, cache_spec, P('dp')), out_specs=(P('dp', None), cache_spec, cache_spec), check_vma=False)
```

```python
import functools
import jax
import jax.numpy as jnp
from jax import lax
from jax.sharding import PartitionSpec as P
from jax.experimental import pallas as pl
from jax.experimental.pallas import tpu as pltpu

MESH = pl.DeviceIdType.MESH
F32 = jnp.float32
BF16 = jnp.bfloat16
HEAD_PAD = 16
BLOCK_ROWS = 8
DMA_ROWS = 16
EARLY = 2
COL_CHUNK = 512
PIECES = (16,) * 4
FIRST_ROWS = 128 - sum(PIECES)
GROUPS = (FIRST_ROWS, 24, 24, 16)
KINDS = ('quarter', 'quarter', 'quarter', 'half')
READ_AHEAD = 6
MIB = 1024 * 1024
ANY_SPEC = pl.BlockSpec(memory_space=pl.ANY)
VMEM_SPEC = pl.BlockSpec(memory_space=pltpu.VMEM)
SMEM_SPEC = pl.BlockSpec(memory_space=pltpu.SMEM)
DMA = pltpu.SemaphoreType.DMA


def patch_rows(buf, new, first, pos_ref, base, rows):
    seq_local, head_dim = buf.shape[-2:]
    sub = lax.broadcasted_iota(jnp.int32, (16, head_dim), 0)
    for i in rows:
        local = pos_ref[first + i] - base
        start = pl.multiple_of(jnp.clip(local // 16, 0, seq_local // 16 - 1) * 16, 16)
        tile = buf[i, pl.ds(start, 16), :].astype(F32)
        row = jnp.broadcast_to(new[pl.ds(first + i, 1), :], (16, head_dim))
        buf[i, pl.ds(start, 16), :] = jnp.where(sub == local - start, row, tile).astype(BF16)


def attend(first, pos_ref, base, scale, q_ref, kb, vb, s_scr, w_scr, o_ref, lane0, o_rows, carry, new=None):
    seq_local, head_dim = kb.shape[-2:]
    n_all = q_ref.shape[1] // HEAD_PAD
    half = head_dim // 2
    lane_t = lax.broadcasted_iota(jnp.int32, (HEAD_PAD, seq_local), 1)
    lane_b = lax.broadcasted_iota(jnp.int32, (HEAD_PAD, 128), 1)
    m_acc, l_acc = carry

    def query(b):
        return jnp.concatenate([q_ref[j, pl.ds(b, HEAD_PAD, stride=n_all), :] for j in range(2)], axis=1)

    for i in range(BLOCK_ROWS):
        s_scr[i] = lax.dot_general(query(first + i).astype(BF16), kb[i], (((1,), (1,)), ((), ())),
                                   preferred_element_type=F32)
    extra = []
    for i in range(BLOCK_ROWS):
        b = first + i
        local = pos_ref[b] - base
        s = s_scr[i]
        if new is not None:
            s_new = jnp.sum(query(b) * new[0][pl.ds(b, 1), :], axis=1, keepdims=True)
            s = jnp.where(lane_t == local, s_new, s)
        s = jnp.where(lane_t <= local, s * scale, -jnp.inf)
        m = jnp.maximum(jnp.max(s, axis=1, keepdims=True), -1e30)
        w = jnp.exp(s - m)
        l = jnp.sum(w, axis=1, keepdims=True)
        if new is not None:
            hit = lane_t == local
            extra.append(jnp.sum(jnp.where(hit, w, 0.0), axis=1, keepdims=True))
            w = jnp.where(hit, 0.0, w)
        w_scr[i] = w.astype(BF16)
        m_acc = jnp.where(lane_b == lane0 + i, m, m_acc)
        l_acc = jnp.where(lane_b == lane0 + i, l, l_acc)
    for i in range(BLOCK_ROWS):
        o = jnp.dot(w_scr[i], vb[i], preferred_element_type=F32)
        if new is not None:
            o = o + extra[i].astype(BF16).astype(F32) * new[1][pl.ds(first + i, 1), :]
        for j in range(2):
            o_ref[pl.ds(j * o_rows + lane0 + i, HEAD_PAD, stride=2 * o_rows), :] = o[:, j * half:(j + 1) * half]
    return m_acc, l_acc


def store_ml(ml_ref, carry):
    ml_ref[pl.ds(0, HEAD_PAD), :] = carry[0]
    ml_ref[pl.ds(HEAD_PAD, HEAD_PAD), :] = carry[1]


def zero_carry():
    return jnp.zeros((HEAD_PAD, 128), F32), jnp.zeros((HEAD_PAD, 128), F32)


def first_kernel(n_heads, pos_ref, tok_hbm, wq_hbm, wk_hbm, wv_hbm, k_hbm, v_hbm,
                 ko_hbm, vo_hbm, q_ref, kn_ref, vn_ref, o_ref, ml_ref,
                 tok, wq, wk, wv, s_scr, w_scr, kbuf, vbuf,
                 w_sems, wq_sems, kin_sems, vin_sems, kout_sems, vout_sems):
    n_rows, seq_local, head_dim = k_hbm.shape
    n_blocks = kbuf.shape[0]
    base = lax.axis_index('sp') * seq_local
    half = head_dim // 2

    def reads(blk):
        rows = pl.ds(blk * DMA_ROWS, DMA_ROWS)
        return (pltpu.make_async_copy(k_hbm.at[rows], kbuf.at[blk], kin_sems.at[blk]),
                pltpu.make_async_copy(v_hbm.at[rows], vbuf.at[blk], vin_sems.at[blk]))

    def writes(blk):
        rows = pl.ds(blk * DMA_ROWS, DMA_ROWS)
        return (pltpu.make_async_copy(kbuf.at[blk], ko_hbm.at[rows], kout_sems.at[blk]),
                pltpu.make_async_copy(vbuf.at[blk], vo_hbm.at[rows], vout_sems.at[blk]))

    small = [pltpu.make_async_copy(s, d, w_sems.at[i])
             for i, (s, d) in enumerate(((tok_hbm, tok), (wk_hbm, wk), (wv_hbm, wv)))]
    n_chunks = wq.shape[1] // COL_CHUNK
    big = [pltpu.make_async_copy(wq_hbm.at[:, pl.ds(i * COL_CHUNK, COL_CHUNK)],
                                 wq.at[:, pl.ds(i * COL_CHUNK, COL_CHUNK)], wq_sems.at[i])
           for i in range(n_chunks)]
    for c in small + big:
        c.start()
    for c in reads(0):
        c.start()
    for j in range(2):
        q_ref[j, pl.ds(n_heads * n_rows, (HEAD_PAD - n_heads) * n_rows), :] = jnp.zeros(
            ((HEAD_PAD - n_heads) * n_rows, half), F32)
    for c in small:
        c.wait()

    def project(w):
        return jnp.dot(tok[...], w, preferred_element_type=F32).astype(BF16).astype(F32)

    kn_ref[...] = project(wk[...])
    vn_ref[...] = project(wv[...])
    per_chunk = COL_CHUNK // head_dim

    def arrive(blk):
        for c in reads(blk):
            c.wait()
        patch_rows(kbuf.at[blk], kn_ref, blk * DMA_ROWS, pos_ref, base, range(DMA_ROWS))
        patch_rows(vbuf.at[blk], vn_ref, blk * DMA_ROWS, pos_ref, base, range(DMA_ROWS))

    for i in range(n_chunks):
        if i + 1 < n_blocks:
            for c in reads(i + 1):
                c.start()
        big[i].wait()
        for h in range(i * per_chunk, (i + 1) * per_chunk):
            q_head = project(wq[:, pl.ds(h * head_dim, head_dim)])
            for j in range(2):
                q_ref[j, pl.ds(h * n_rows, n_rows), :] = q_head[:, j * half:(j + 1) * half]
    for blk in range(n_chunks + 1, n_blocks):
        for c in reads(blk):
            c.start()

    def block(blk, carry):
        for j in range(DMA_ROWS // BLOCK_ROWS):
            first = blk * DMA_ROWS + j * BLOCK_ROWS
            rows = pl.ds(j * BLOCK_ROWS, BLOCK_ROWS)
            carry = attend(first, pos_ref, base, head_dim ** -0.5, q_ref, kbuf.at[blk, rows], vbuf.at[blk, rows],
                           s_scr, w_scr, o_ref, first, n_blocks * DMA_ROWS, carry)
        return carry

    def early_block(blk, carry):
        arrive(blk)
        return block(blk, carry)

    carry = lax.fori_loop(0, EARLY, early_block, zero_carry())
    for blk in range(EARLY, n_blocks):
        arrive(blk)
    for blk in range(n_blocks):
        for c in writes(blk):
            c.start()
    store_ml(ml_ref, lax.fori_loop(EARLY, n_blocks, block, carry))
    for blk in range(n_blocks):
        for c in writes(blk):
            c.wait()


def first_part(pos, tok, wq, wk, wv, k, v):
    n_rows, seq_local, head_dim = k.shape
    d_model, q_width = wq.shape
    n_heads = q_width // head_dim
    n_blocks = FIRST_ROWS // DMA_ROWS
    block = pltpu.VMEM((n_blocks, DMA_ROWS, seq_local, head_dim), BF16)
    return pl.pallas_call(
        functools.partial(first_kernel, n_heads),
        out_shape=(jax.ShapeDtypeStruct(k.shape, k.dtype), jax.ShapeDtypeStruct(v.shape, v.dtype),
                   pltpu.VMEM((2, HEAD_PAD * n_rows, head_dim // 2), F32),
                   pltpu.VMEM((n_rows, head_dim), F32), pltpu.VMEM((n_rows, head_dim), F32),
                   pltpu.VMEM((2 * HEAD_PAD * FIRST_ROWS, head_dim // 2), F32),
                   pltpu.VMEM((2 * HEAD_PAD, 128), F32)),
        in_specs=[SMEM_SPEC] + [ANY_SPEC] * 6,
        out_specs=(ANY_SPEC, ANY_SPEC) + (VMEM_SPEC,) * 5,
        scratch_shapes=[
            pltpu.VMEM(tok.shape, BF16), pltpu.VMEM(wq.shape, BF16),
            pltpu.VMEM(wk.shape, BF16), pltpu.VMEM(wv.shape, BF16),
            pltpu.VMEM((BLOCK_ROWS, HEAD_PAD, seq_local), F32),
            pltpu.VMEM((BLOCK_ROWS, HEAD_PAD, seq_local), BF16),
            block, block,
            DMA((3,)), DMA((q_width // COL_CHUNK,)),
            DMA((n_blocks,)), DMA((n_blocks,)), DMA((n_blocks,)), DMA((n_blocks,))],
        compiler_params=pltpu.CompilerParams(vmem_limit_bytes=60 * MIB),
        cost_estimate=pl.CostEstimate(flops=10**10, bytes_accessed=70 * 10**6, transcendentals=0),
        name='attention_first',
    )(pos, tok, wq, wk, wv, k, v)


COPIES = 10
N_PIECES = len(PIECES)
PIECE_ROW0 = tuple(sum(PIECES[:i]) for i in range(N_PIECES))


class Group:
    def __init__(self):
        self.copies = {}

    def __getattr__(self, name):
        return self.__dict__['copies'][name]()


def rest_kernel(pos_ref, q_ref, kn_ref, vn_ref, o0, ml0, wo_hbm, k_hbm, v_hbm,
                *refs):
    kret, vret = refs[:N_PIECES], refs[N_PIECES:2 * N_PIECES]
    rest_body(pos_ref, q_ref, kn_ref, vn_ref, o0, ml0, wo_hbm, k_hbm, v_hbm, kret, vret, *refs[2 * N_PIECES:])


def rest_body(pos_ref, q_ref, kn_ref, vn_ref, o0, ml0, wo_hbm, k_hbm, v_hbm,
              kret, vret, y_ref, wo, s_scr, w_scr, fbuf, wo_sem, kin_sems, vin_sems, send, recv, *scratch):
    n_rows, seq_local, head_dim = k_hbm.shape
    rows_local, d_model = wo.shape
    units = rows_local // 128
    half_width = d_model // 2
    n_blocks = sum(PIECES) // BLOCK_ROWS
    me = lax.axis_index('sp')
    base = me * seq_local
    core = lax.rem(me, 2)
    chip = me // 2
    partner = chip * 2 + 1 - core
    cross = (1 - chip) * 2 + core
    far, near = (1 - chip) * 2, chip * 2

    def reads(blk):
        p = piece_of(blk)
        src = pl.ds(FIRST_ROWS + blk * BLOCK_ROWS, BLOCK_ROWS)
        dst = pl.ds(blk * BLOCK_ROWS - PIECE_ROW0[p], BLOCK_ROWS)
        return (pltpu.make_async_copy(k_hbm.at[src], kret[p].at[dst], kin_sems.at[blk]),
                pltpu.make_async_copy(v_hbm.at[src], vret[p].at[dst], vin_sems.at[blk]))

    barrier = pltpu.get_barrier_semaphore()
    for peer in (partner, cross):
        pl.semaphore_signal(barrier, inc=1, device_id={'sp': peer}, device_id_type=MESH)
    for blk in range(min(READ_AHEAD, n_blocks)):
        for c in reads(blk):
            c.start()
    load_wo = pltpu.make_async_copy(wo_hbm, wo, wo_sem)
    load_wo.start()

    def group(idx):
        g = Group()
        g.n, g.row0 = GROUPS[idx], sum(GROUPS[:idx])
        refs = scratch[idx * len(BUFS):(idx + 1) * len(BUFS)]
        for name, ref in zip(BUFS, refs):
            setattr(g, name, ref)
        if idx == 0:
            g.o, g.ml = o0, ml0
        g.span = units * g.n

        def remote(i, src, dst, peer):
            return pltpu.make_async_remote_copy(src_ref=src, dst_ref=dst, send_sem=send.at[idx, i],
                                                recv_sem=recv.at[idx, i], device_id={'sp': peer},
                                                device_id_type=MESH)

        def part(dest):
            return g.o.at[pl.ds(pl.multiple_of(dest * g.span, 8), g.span)]

        g.copies['p_ml'] = lambda: remote(0, g.ml, g.pml, partner)
        g.copies['p_far'] = lambda: remote(1, part(far + 1 - core), g.po.at[0], partner)
        g.copies['p_near'] = lambda: remote(2, part(near + 1 - core), g.po.at[1], partner)
        g.copies['x_ml'] = lambda: remote(3, g.mlc, g.xml, cross)
        g.copies['x_o'] = lambda: remote(4, g.oc, g.xo, cross)
        g.copies['p_y'] = lambda: remote(5, g.yq, g.yp, partner)
        g.copies['x_y'] = lambda: remote(6, g.yx, g.yxr, cross)
        if KINDS[idx] == 'half':
            g.copies['p_b'] = lambda: remote(7, g.yb, g.yg, partner)
        else:
            g.copies['p_b'] = lambda: remote(7, g.yb, g.yg.at[1], partner)
            g.copies['x_b'] = lambda: remote(8, g.yb, g.yg.at[0], cross)
            g.copies['p_f'] = lambda: remote(9, g.yg.at[0], g.yg.at[2], partner)
        return g

    def merge(a, b):
        n = a.shape[0] // 2
        peak = jnp.maximum(a[:n], b[:n])
        fa = jnp.exp(a[:n] - peak)
        fb = jnp.exp(b[:n] - peak)
        return fa, fb, peak, a[n:] * fa + b[n:] * fb

    def picks(k, dest):
        rows = [fbuf[k, pl.ds((dest * units + u) // 2, 1), :] for u in range(units)]
        return jnp.concatenate(rows + [rows[-1]] * (8 - units), axis=0)

    def stage0(g):
        for c in (g.p_ml, g.p_far, g.p_near):
            c.start()

    def stage1(g):
        g.p_ml.wait_recv()
        for k, value in enumerate(merge(g.ml[...], g.pml[...])):
            fbuf[k] = value
        for ref, dest in ((g.mlc, far + core), (g.mlo, me)):
            ref[pl.ds(0, 8), :] = picks(2, dest)
            ref[pl.ds(8, 8), :] = picks(3, dest)
        g.x_ml.start()

        def chip_part(dest, slot, dst):
            ca, cb = picks(0, dest).T[:g.n], picks(1, dest).T[:g.n]
            for u in range(units):
                mine = g.o[pl.ds(pl.multiple_of(dest * g.span + u * g.n, 8), g.n), :]
                theirs = g.po[slot, pl.ds(u * g.n, g.n), :]
                dst[pl.ds(u * g.n, g.n), :] = mine * ca[:, u:u + 1] + theirs * cb[:, u:u + 1]

        g.p_far.wait_recv()
        chip_part(far + core, 0, g.oc)
        g.x_o.start()
        g.p_near.wait_recv()
        chip_part(me, 1, g.om)

    def stage2(g):
        g.x_ml.wait_recv()
        fa, fb, _, total = merge(g.mlo[...], g.xml[...])
        ca, cb, cl = fa.T[:g.n], fb.T[:g.n], total.T[:g.n]
        g.x_o.wait_recv()
        for u in range(units):
            rows = pl.ds(u * g.n, g.n)
            value = g.om[rows, :] * ca[:, u:u + 1] + g.xo[rows, :] * cb[:, u:u + 1]
            g.ob[:, u * 128:(u + 1) * 128] = (value / cl[:, u:u + 1]).astype(BF16)

        def product(c):
            cols = pl.ds(pl.multiple_of(c * half_width, 128), half_width)
            return jnp.dot(g.ob[...], wo[:, cols], preferred_element_type=F32)

        g.yq[...] = product(1 - core)
        g.p_y.start()
        g.ym[...] = product(core)

    def place(g, start, value):
        width = value.shape[1]
        y_ref[pl.ds(g.row0, g.n), pl.ds(pl.multiple_of(start, 128), width)] = value

    def stage3_half(g):
        g.p_y.wait_recv()
        g.yx[...] = g.ym[...] + g.yp[...]
        g.x_y.start()

    def stage4_half(g):
        g.x_y.wait_recv()
        g.yb[...] = (g.yx[...] + g.yxr[...]).astype(BF16)
        g.p_b.start()
        place(g, core * half_width, g.yb[...])

    def finish(g):
        for name in g.copies:
            g.copies[name]().wait_send()

    def stage5_half(g):
        g.p_b.wait_recv()
        place(g, (1 - core) * half_width, g.yg[...])
        finish(g)

    quarter = half_width // 2
    far_cols = pl.ds(pl.multiple_of((1 - chip) * quarter, 128), quarter)
    near_cols = pl.ds(pl.multiple_of(chip * quarter, 128), quarter)

    def stage3_quarter(g):
        g.p_y.wait_recv()
        g.yx[...] = g.ym[:, far_cols] + g.yp[:, far_cols]
        g.x_y.start()
        g.yn[...] = g.ym[:, near_cols] + g.yp[:, near_cols]

    def stage4_quarter(g):
        g.x_y.wait_recv()
        g.yb[...] = (g.yn[...] + g.yxr[...]).astype(BF16)
        g.x_b.start()
        g.p_b.start()
        place(g, core * half_width + chip * quarter, g.yb[...])

    def stage5_quarter(g):
        g.x_b.wait_recv()
        g.p_f.start()
        place(g, core * half_width + (1 - chip) * quarter, g.yg[0])

    def stage6_quarter(g):
        g.p_b.wait_recv()
        place(g, (1 - core) * half_width + chip * quarter, g.yg[1])
        g.p_f.wait_recv()
        place(g, (1 - core) * half_width + (1 - chip) * quarter, g.yg[2])
        finish(g)

    common = (stage0, stage1, stage2)
    stages = dict(half=common + (stage3_half, stage4_half, stage5_half),
                  quarter=common + (stage3_quarter, stage4_quarter, stage5_quarter, stage6_quarter))
    groups = [group(i) for i in range(len(GROUPS))]

    def attend_block(blk):
        if blk + READ_AHEAD < n_blocks:
            for c in reads(blk + READ_AHEAD):
                c.start()
        for c in reads(blk):
            c.wait()
        p = piece_of(blk)
        row = FIRST_ROWS + blk * BLOCK_ROWS
        idx = [i for i in range(len(GROUPS)) if row >= sum(GROUPS[:i])][-1]
        g = groups[idx]
        lane0 = row - g.row0
        carry = zero_carry() if lane0 == 0 else (g.ml[pl.ds(0, HEAD_PAD), :], g.ml[pl.ds(HEAD_PAD, HEAD_PAD), :])
        rows = pl.ds(blk * BLOCK_ROWS - PIECE_ROW0[p], BLOCK_ROWS)
        store_ml(g.ml, attend(row, pos_ref, base, head_dim ** -0.5, q_ref, kret[p].at[rows], vret[p].at[rows],
                              s_scr, w_scr, g.o, lane0, g.n, carry, (kn_ref, vn_ref)))

    for action in SCHEDULE:
        if isinstance(action, int):
            attend_block(action)
        elif action == 'wo':
            load_wo.wait()
        elif action == 'barrier':
            pl.semaphore_wait(barrier, 2)
        else:
            stages[KINDS[action[0]]][action[1]](groups[action[0]])


def piece_of(blk):
    return [i for i in range(N_PIECES) if blk * BLOCK_ROWS >= PIECE_ROW0[i]][-1]


BUFS = ('o', 'ml', 'pml', 'po', 'mlc', 'mlo', 'oc', 'om', 'xo', 'xml', 'ob', 'yq', 'yp', 'ym', 'yn', 'yx', 'yxr', 'yb',
        'yg')
SCHEDULE = ('barrier', (0, 0), 0, (0, 1), 1, 2, (1, 0), 3, (1, 1), 4, 5, (2, 0), 'wo', (0, 2), (2, 1), 6, (0,
            3), 7, (3, 0), (1, 2), (3, 1), (2, 2), (1, 3), (2, 3), (0, 4), (3, 2), (1, 4), (3, 3), (2, 4), (1,
            5), (1, 6), (0, 5), (3, 4), (2, 5), (3, 5), (0, 6), (2, 6))


def rest_part(pos, q, kn, vn, o0, ml0, wo, k, v):
    n_rows, seq_local, head_dim = k.shape
    rows_local, d_model = wo.shape
    units = rows_local // 128
    n_blocks = sum(PIECES) // BLOCK_ROWS

    def buffers(n, own, kind):
        span = units * n
        ml, part, half = (2 * HEAD_PAD, 128), (span, 128), (n, d_model // 2)
        slab = half if kind == 'half' else (n, d_model // 4)
        shapes = dict(o=((2 * HEAD_PAD * n if own else 8, 128), F32), ml=(ml, F32),
                      pml=(ml, F32), po=((2,) + part, F32), mlc=((16, 128), F32), mlo=((16, 128), F32), oc=(part, F32), om=(part, F32),
                      xo=(part, F32), xml=((16, 128), F32), ob=((n, rows_local), BF16), yq=(half, F32), yp=(half, F32),
                      ym=(half, F32), yn=(slab if kind != 'half' else (8, 128), F32), yx=(slab, F32),
                      yxr=(slab, F32), yb=(slab, BF16), yg=(slab if kind == 'half' else (3,) + slab, BF16))
        return [pltpu.VMEM(*shapes[name]) for name in BUFS]

    return pl.pallas_call(
        rest_kernel,
        out_shape=tuple(pltpu.VMEM((n, seq_local, head_dim), BF16) for n in PIECES * 2)
        + (pltpu.VMEM((n_rows, d_model), BF16),),
        in_specs=[SMEM_SPEC] + [VMEM_SPEC] * 5 + [ANY_SPEC] * 3,
        out_specs=(VMEM_SPEC,) * (2 * N_PIECES + 1),
        scratch_shapes=[
            pltpu.VMEM(wo.shape, BF16),
            pltpu.VMEM((BLOCK_ROWS, HEAD_PAD, seq_local), F32),
            pltpu.VMEM((BLOCK_ROWS, HEAD_PAD, seq_local), BF16),
            pltpu.VMEM((4, HEAD_PAD, 128), F32),
            DMA, DMA((n_blocks,)), DMA((n_blocks,)), DMA((len(GROUPS), COPIES)), DMA((len(GROUPS), COPIES))]
            + [b for i, n in enumerate(GROUPS) for b in buffers(n, i > 0, KINDS[i])],
        compiler_params=pltpu.CompilerParams(collective_id=0, has_side_effects=True, vmem_limit_bytes=REST_VMEM * MIB),
        cost_estimate=pl.CostEstimate(flops=10**10, bytes_accessed=40 * 10**6, transcendentals=0),
        name='attention_rest',
    )(pos, q, kn, vn, o0, ml0, wo, k, v)


REST_VMEM = 18


def write_kernel(pos_ref, kn_ref, vn_ref, y_ref, *refs):
    ko_hbm, vo_hbm, y_hbm = refs[2 * N_PIECES + 2:2 * N_PIECES + 5]
    kret, vret = refs[2 * N_PIECES + 5:3 * N_PIECES + 5], refs[3 * N_PIECES + 5:4 * N_PIECES + 5]
    k_sems, v_sems, y_sem = refs[4 * N_PIECES + 5:]
    seq_local = ko_hbm.shape[1]
    base = lax.axis_index('sp') * seq_local
    write_y = pltpu.make_async_copy(y_ref, y_hbm, y_sem)

    def writes(p):
        dst = pl.ds(FIRST_ROWS + PIECE_ROW0[p], PIECES[p])
        return (pltpu.make_async_copy(kret[p], ko_hbm.at[dst], k_sems.at[p]),
                pltpu.make_async_copy(vret[p], vo_hbm.at[dst], v_sems.at[p]))

    for p in range(N_PIECES):
        for kept, new, copy in zip((kret, vret), (kn_ref, vn_ref), writes(p)):
            patch_rows(kept[p], new, FIRST_ROWS + PIECE_ROW0[p], pos_ref, base, range(PIECES[p]))
            copy.start()
    write_y.start()
    write_y.wait()
    for p in range(N_PIECES):
        for c in writes(p):
            c.wait()


def write_part(pos, kn, vn, y, ko, vo, kret, vret):
    kept = (*kret, *vret)
    out = pl.pallas_call(
        write_kernel,
        out_shape=(jax.ShapeDtypeStruct(ko.shape, ko.dtype), jax.ShapeDtypeStruct(vo.shape, vo.dtype),
                   jax.ShapeDtypeStruct(y.shape, y.dtype)) + tuple(pltpu.VMEM(a.shape, a.dtype) for a in kept),
        in_specs=[SMEM_SPEC, VMEM_SPEC, VMEM_SPEC, VMEM_SPEC] + [VMEM_SPEC] * (2 * N_PIECES) + [ANY_SPEC, ANY_SPEC],
        out_specs=(ANY_SPEC, ANY_SPEC, ANY_SPEC) + (VMEM_SPEC,) * (2 * N_PIECES),
        input_output_aliases={4 + 2 * N_PIECES: 0, 5 + 2 * N_PIECES: 1,
                              **{4 + i: 3 + i for i in range(2 * N_PIECES)}},
        scratch_shapes=[DMA((N_PIECES,)), DMA((N_PIECES,)), DMA],
        compiler_params=pltpu.CompilerParams(vmem_limit_bytes=REST_VMEM * MIB),
        cost_estimate=pl.CostEstimate(flops=10**10, bytes_accessed=40 * 10**6, transcendentals=0),
        name='attention_write',
    )(pos, kn, vn, y, *kept, ko, vo)
    return out[2], out[0], out[1]


def in_vmem(*arrays):
    return [pltpu.with_memory_space_constraint(a, pltpu.VMEM) for a in arrays]


def solution(mesh):
    def local_step(tokens, w_query, w_key, w_value, w_out, k_cache, v_cache, positions):
        ko, vo, q, kn, vn, o0, ml0 = first_part(
            positions, tokens, w_query, w_key, w_value, k_cache, v_cache)
        q, kn, vn, o0, ml0 = in_vmem(q, kn, vn, o0, ml0)
        *kept, y = rest_part(positions, q, kn, vn, o0, ml0, w_out, k_cache, v_cache)
        *kept, y = in_vmem(*kept, y)
        return write_part(positions, kn, vn, y, ko, vo, kept[:N_PIECES], kept[N_PIECES:])

    cache_spec = P('dp', 'sp', None)
    return jax.shard_map(local_step, mesh=mesh, in_specs=(P('dp', None), P(), P(), P(), P('sp', None), cache_spec, cache_spec, P('dp')), out_specs=(P('dp', None), cache_spec, cache_spec), check_vma=False)
```

```python
import functools
import jax
import jax.numpy as jnp
from jax import lax
from jax.sharding import PartitionSpec as P
from jax.experimental import pallas as pl
from jax.experimental.pallas import tpu as pltpu

MESH = pl.DeviceIdType.MESH
F32 = jnp.float32
BF16 = jnp.bfloat16
HEAD_PAD = 16
BLOCK_ROWS = 8
DMA_ROWS = 8
EARLY = 5
COL_CHUNK = 512
PIECES = (16,) * 4
FIRST_ROWS = 128 - sum(PIECES)
GROUPS = (FIRST_ROWS, 24, 24, 16)
KINDS = ('quarter', 'quarter', 'quarter', 'half')
READ_AHEAD = 6
MIB = 1024 * 1024
ANY_SPEC = pl.BlockSpec(memory_space=pl.ANY)
VMEM_SPEC = pl.BlockSpec(memory_space=pltpu.VMEM)
SMEM_SPEC = pl.BlockSpec(memory_space=pltpu.SMEM)
DMA = pltpu.SemaphoreType.DMA


def patch_rows(buf, new, first, pos_ref, base, rows):
    seq_local, head_dim = buf.shape[-2:]
    sub = lax.broadcasted_iota(jnp.int32, (16, head_dim), 0)
    for i in rows:
        local = pos_ref[first + i] - base
        start = pl.multiple_of(jnp.clip(local // 16, 0, seq_local // 16 - 1) * 16, 16)
        tile = buf[i, pl.ds(start, 16), :].astype(F32)
        row = jnp.broadcast_to(new[pl.ds(first + i, 1), :], (16, head_dim))
        buf[i, pl.ds(start, 16), :] = jnp.where(sub == local - start, row, tile).astype(BF16)


def attend(first, pos_ref, base, scale, q_ref, kb, vb, s_scr, w_scr, o_ref, lane0, o_rows, carry, new=None):
    seq_local, head_dim = kb.shape[-2:]
    n_all = q_ref.shape[1] // HEAD_PAD
    half = head_dim // 2
    lane_t = lax.broadcasted_iota(jnp.int32, (HEAD_PAD, seq_local), 1)
    lane_b = lax.broadcasted_iota(jnp.int32, (HEAD_PAD, 128), 1)
    m_acc, l_acc = carry

    def query(b):
        return jnp.concatenate([q_ref[j, pl.ds(b, HEAD_PAD, stride=n_all), :] for j in range(2)], axis=1)

    for i in range(BLOCK_ROWS):
        s_scr[i] = lax.dot_general(query(first + i).astype(BF16), kb[i], (((1,), (1,)), ((), ())),
                                   preferred_element_type=F32)
    extra = []
    for i in range(BLOCK_ROWS):
        b = first + i
        local = pos_ref[b] - base
        s = s_scr[i]
        if new is not None:
            s_new = jnp.sum(query(b) * new[0][pl.ds(b, 1), :], axis=1, keepdims=True)
            s = jnp.where(lane_t == local, s_new, s)
        s = jnp.where(lane_t <= local, s * scale, -jnp.inf)
        m = jnp.maximum(jnp.max(s, axis=1, keepdims=True), -1e30)
        w = jnp.exp(s - m)
        l = jnp.sum(w, axis=1, keepdims=True)
        if new is not None:
            hit = lane_t == local
            extra.append(jnp.sum(jnp.where(hit, w, 0.0), axis=1, keepdims=True))
            w = jnp.where(hit, 0.0, w)
        w_scr[i] = w.astype(BF16)
        m_acc = jnp.where(lane_b == lane0 + i, m, m_acc)
        l_acc = jnp.where(lane_b == lane0 + i, l, l_acc)
    for i in range(BLOCK_ROWS):
        o = jnp.dot(w_scr[i], vb[i], preferred_element_type=F32)
        if new is not None:
            o = o + extra[i].astype(BF16).astype(F32) * new[1][pl.ds(first + i, 1), :]
        for j in range(2):
            o_ref[pl.ds(j * o_rows + lane0 + i, HEAD_PAD, stride=2 * o_rows), :] = o[:, j * half:(j + 1) * half]
    return m_acc, l_acc


def store_ml(ml_ref, carry):
    ml_ref[pl.ds(0, HEAD_PAD), :] = carry[0]
    ml_ref[pl.ds(HEAD_PAD, HEAD_PAD), :] = carry[1]


def zero_carry():
    return jnp.zeros((HEAD_PAD, 128), F32), jnp.zeros((HEAD_PAD, 128), F32)


def first_kernel(n_heads, pos_ref, tok_hbm, wq_hbm, wk_hbm, wv_hbm, k_hbm, v_hbm,
                 ko_hbm, vo_hbm, q_ref, kn_ref, vn_ref, o_ref, ml_ref,
                 tok, wq, wk, wv, s_scr, w_scr, kbuf, vbuf,
                 w_sems, wq_sems, kin_sems, vin_sems, kout_sems, vout_sems):
    n_rows, seq_local, head_dim = k_hbm.shape
    n_blocks = kbuf.shape[0]
    base = lax.axis_index('sp') * seq_local
    half = head_dim // 2

    def reads(blk):
        rows = pl.ds(blk * DMA_ROWS, DMA_ROWS)
        return (pltpu.make_async_copy(k_hbm.at[rows], kbuf.at[blk], kin_sems.at[blk]),
                pltpu.make_async_copy(v_hbm.at[rows], vbuf.at[blk], vin_sems.at[blk]))

    def writes(blk):
        rows = pl.ds(blk * DMA_ROWS, DMA_ROWS)
        return (pltpu.make_async_copy(kbuf.at[blk], ko_hbm.at[rows], kout_sems.at[blk]),
                pltpu.make_async_copy(vbuf.at[blk], vo_hbm.at[rows], vout_sems.at[blk]))

    small = [pltpu.make_async_copy(s, d, w_sems.at[i])
             for i, (s, d) in enumerate(((tok_hbm, tok), (wk_hbm, wk), (wv_hbm, wv)))]
    n_chunks = wq.shape[1] // COL_CHUNK
    big = [pltpu.make_async_copy(wq_hbm.at[:, pl.ds(i * COL_CHUNK, COL_CHUNK)],
                                 wq.at[:, pl.ds(i * COL_CHUNK, COL_CHUNK)], wq_sems.at[i])
           for i in range(n_chunks)]
    for c in small + big:
        c.start()
    for c in reads(0):
        c.start()
    for j in range(2):
        q_ref[j, pl.ds(n_heads * n_rows, (HEAD_PAD - n_heads) * n_rows), :] = jnp.zeros(
            ((HEAD_PAD - n_heads) * n_rows, half), F32)
    for c in small:
        c.wait()

    def project(w):
        return jnp.dot(tok[...], w, preferred_element_type=F32).astype(BF16).astype(F32)

    kn_ref[...] = project(wk[...])
    vn_ref[...] = project(wv[...])
    per_chunk = COL_CHUNK // head_dim

    def arrive(blk):
        for c in reads(blk):
            c.wait()
        patch_rows(kbuf.at[blk], kn_ref, blk * DMA_ROWS, pos_ref, base, range(DMA_ROWS))
        patch_rows(vbuf.at[blk], vn_ref, blk * DMA_ROWS, pos_ref, base, range(DMA_ROWS))

    for i in range(n_chunks):
        if i + 1 < n_blocks:
            for c in reads(i + 1):
                c.start()
        big[i].wait()
        for h in range(i * per_chunk, (i + 1) * per_chunk):
            q_head = project(wq[:, pl.ds(h * head_dim, head_dim)])
            for j in range(2):
                q_ref[j, pl.ds(h * n_rows, n_rows), :] = q_head[:, j * half:(j + 1) * half]
    for blk in range(n_chunks + 1, n_blocks):
        for c in reads(blk):
            c.start()

    def block(blk, carry):
        for j in range(DMA_ROWS // BLOCK_ROWS):
            first = blk * DMA_ROWS + j * BLOCK_ROWS
            rows = pl.ds(j * BLOCK_ROWS, BLOCK_ROWS)
            carry = attend(first, pos_ref, base, head_dim ** -0.5, q_ref, kbuf.at[blk, rows], vbuf.at[blk, rows],
                           s_scr, w_scr, o_ref, first, n_blocks * DMA_ROWS, carry)
        return carry

    def early_block(blk, carry):
        arrive(blk)
        return block(blk, carry)

    carry = lax.fori_loop(0, EARLY, early_block, zero_carry())
    for blk in range(EARLY, n_blocks):
        arrive(blk)
    for blk in range(n_blocks):
        for c in writes(blk):
            c.start()
    store_ml(ml_ref, lax.fori_loop(EARLY, n_blocks, block, carry))
    for blk in range(n_blocks):
        for c in writes(blk):
            c.wait()


def first_part(pos, tok, wq, wk, wv, k, v):
    n_rows, seq_local, head_dim = k.shape
    d_model, q_width = wq.shape
    n_heads = q_width // head_dim
    n_blocks = FIRST_ROWS // DMA_ROWS
    block = pltpu.VMEM((n_blocks, DMA_ROWS, seq_local, head_dim), BF16)
    return pl.pallas_call(
        functools.partial(first_kernel, n_heads),
        out_shape=(jax.ShapeDtypeStruct(k.shape, k.dtype), jax.ShapeDtypeStruct(v.shape, v.dtype),
                   pltpu.VMEM((2, HEAD_PAD * n_rows, head_dim // 2), F32),
                   pltpu.VMEM((n_rows, head_dim), F32), pltpu.VMEM((n_rows, head_dim), F32),
                   pltpu.VMEM((2 * HEAD_PAD * FIRST_ROWS, head_dim // 2), F32),
                   pltpu.VMEM((2 * HEAD_PAD, 128), F32)),
        in_specs=[SMEM_SPEC] + [ANY_SPEC] * 6,
        out_specs=(ANY_SPEC, ANY_SPEC) + (VMEM_SPEC,) * 5,
        scratch_shapes=[
            pltpu.VMEM(tok.shape, BF16), pltpu.VMEM(wq.shape, BF16),
            pltpu.VMEM(wk.shape, BF16), pltpu.VMEM(wv.shape, BF16),
            pltpu.VMEM((BLOCK_ROWS, HEAD_PAD, seq_local), F32),
            pltpu.VMEM((BLOCK_ROWS, HEAD_PAD, seq_local), BF16),
            block, block,
            DMA((3,)), DMA((q_width // COL_CHUNK,)),
            DMA((n_blocks,)), DMA((n_blocks,)), DMA((n_blocks,)), DMA((n_blocks,))],
        compiler_params=pltpu.CompilerParams(vmem_limit_bytes=60 * MIB),
        cost_estimate=pl.CostEstimate(flops=10**10, bytes_accessed=70 * 10**6, transcendentals=0),
        name='attention_first',
    )(pos, tok, wq, wk, wv, k, v)


COPIES = 10
N_PIECES = len(PIECES)
PIECE_ROW0 = tuple(sum(PIECES[:i]) for i in range(N_PIECES))


class Group:
    def __init__(self):
        self.copies = {}

    def __getattr__(self, name):
        return self.__dict__['copies'][name]()


def rest_kernel(pos_ref, q_ref, kn_ref, vn_ref, o0, ml0, wo_hbm, k_hbm, v_hbm,
                *refs):
    kret, vret = refs[:N_PIECES], refs[N_PIECES:2 * N_PIECES]
    rest_body(pos_ref, q_ref, kn_ref, vn_ref, o0, ml0, wo_hbm, k_hbm, v_hbm, kret, vret, *refs[2 * N_PIECES:])


def rest_body(pos_ref, q_ref, kn_ref, vn_ref, o0, ml0, wo_hbm, k_hbm, v_hbm,
              kret, vret, y_ref, wo, s_scr, w_scr, fbuf, wo_sem, kin_sems, vin_sems, send, recv, *scratch):
    n_rows, seq_local, head_dim = k_hbm.shape
    rows_local, d_model = wo.shape
    units = rows_local // 128
    half_width = d_model // 2
    n_blocks = sum(PIECES) // BLOCK_ROWS
    me = lax.axis_index('sp')
    base = me * seq_local
    core = lax.rem(me, 2)
    chip = me // 2
    partner = chip * 2 + 1 - core
    cross = (1 - chip) * 2 + core
    far, near = (1 - chip) * 2, chip * 2

    def reads(blk):
        p = piece_of(blk)
        src = pl.ds(FIRST_ROWS + blk * BLOCK_ROWS, BLOCK_ROWS)
        dst = pl.ds(blk * BLOCK_ROWS - PIECE_ROW0[p], BLOCK_ROWS)
        return (pltpu.make_async_copy(k_hbm.at[src], kret[p].at[dst], kin_sems.at[blk]),
                pltpu.make_async_copy(v_hbm.at[src], vret[p].at[dst], vin_sems.at[blk]))

    barrier = pltpu.get_barrier_semaphore()
    for peer in (partner, cross):
        pl.semaphore_signal(barrier, inc=1, device_id={'sp': peer}, device_id_type=MESH)
    for blk in range(min(READ_AHEAD, n_blocks)):
        for c in reads(blk):
            c.start()
    load_wo = pltpu.make_async_copy(wo_hbm, wo, wo_sem)
    load_wo.start()

    def group(idx):
        g = Group()
        g.n, g.row0 = GROUPS[idx], sum(GROUPS[:idx])
        refs = scratch[idx * len(BUFS):(idx + 1) * len(BUFS)]
        for name, ref in zip(BUFS, refs):
            setattr(g, name, ref)
        if idx == 0:
            g.o, g.ml = o0, ml0
        g.span = units * g.n

        def remote(i, src, dst, peer):
            return pltpu.make_async_remote_copy(src_ref=src, dst_ref=dst, send_sem=send.at[idx, i],
                                                recv_sem=recv.at[idx, i], device_id={'sp': peer},
                                                device_id_type=MESH)

        def part(dest):
            return g.o.at[pl.ds(pl.multiple_of(dest * g.span, 8), g.span)]

        g.copies['p_ml'] = lambda: remote(0, g.ml, g.pml, partner)
        g.copies['p_far'] = lambda: remote(1, part(far + 1 - core), g.po.at[0], partner)
        g.copies['p_near'] = lambda: remote(2, part(near + 1 - core), g.po.at[1], partner)
        g.copies['x_ml'] = lambda: remote(3, g.mlc, g.xml, cross)
        g.copies['x_o'] = lambda: remote(4, g.oc, g.xo, cross)
        g.copies['p_y'] = lambda: remote(5, g.yq, g.yp, partner)
        g.copies['x_y'] = lambda: remote(6, g.yx, g.yxr, cross)
        if KINDS[idx] == 'half':
            g.copies['p_b'] = lambda: remote(7, g.yb, g.yg, partner)
        else:
            g.copies['p_b'] = lambda: remote(7, g.yb, g.yg.at[1], partner)
            g.copies['x_b'] = lambda: remote(8, g.yb, g.yg.at[0], cross)
            g.copies['p_f'] = lambda: remote(9, g.yg.at[0], g.yg.at[2], partner)
        return g

    def merge(a, b):
        n = a.shape[0] // 2
        peak = jnp.maximum(a[:n], b[:n])
        fa = jnp.exp(a[:n] - peak)
        fb = jnp.exp(b[:n] - peak)
        return fa, fb, peak, a[n:] * fa + b[n:] * fb

    def picks(k, dest):
        rows = [fbuf[k, pl.ds((dest * units + u) // 2, 1), :] for u in range(units)]
        return jnp.concatenate(rows + [rows[-1]] * (8 - units), axis=0)

    def stage0(g):
        for c in (g.p_ml, g.p_far, g.p_near):
            c.start()

    def stage1(g):
        g.p_ml.wait_recv()
        for k, value in enumerate(merge(g.ml[...], g.pml[...])):
            fbuf[k] = value
        for ref, dest in ((g.mlc, far + core), (g.mlo, me)):
            ref[pl.ds(0, 8), :] = picks(2, dest)
            ref[pl.ds(8, 8), :] = picks(3, dest)
        g.x_ml.start()

        def chip_part(dest, slot, dst):
            ca, cb = picks(0, dest).T[:g.n], picks(1, dest).T[:g.n]
            for u in range(units):
                mine = g.o[pl.ds(pl.multiple_of(dest * g.span + u * g.n, 8), g.n), :]
                theirs = g.po[slot, pl.ds(u * g.n, g.n), :]
                dst[pl.ds(u * g.n, g.n), :] = mine * ca[:, u:u + 1] + theirs * cb[:, u:u + 1]

        g.p_far.wait_recv()
        chip_part(far + core, 0, g.oc)
        g.x_o.start()
        g.p_near.wait_recv()
        chip_part(me, 1, g.om)

    def stage2(g):
        g.x_ml.wait_recv()
        fa, fb, _, total = merge(g.mlo[...], g.xml[...])
        ca, cb, cl = fa.T[:g.n], fb.T[:g.n], total.T[:g.n]
        g.x_o.wait_recv()
        for u in range(units):
            rows = pl.ds(u * g.n, g.n)
            value = g.om[rows, :] * ca[:, u:u + 1] + g.xo[rows, :] * cb[:, u:u + 1]
            g.ob[:, u * 128:(u + 1) * 128] = (value / cl[:, u:u + 1]).astype(BF16)

        def product(c):
            cols = pl.ds(pl.multiple_of(c * half_width, 128), half_width)
            return jnp.dot(g.ob[...], wo[:, cols], preferred_element_type=F32)

        g.yq[...] = product(1 - core)
        g.p_y.start()
        g.ym[...] = product(core)

    def place(g, start, value):
        width = value.shape[1]
        y_ref[pl.ds(g.row0, g.n), pl.ds(pl.multiple_of(start, 128), width)] = value

    def stage3_half(g):
        g.p_y.wait_recv()
        g.yx[...] = g.ym[...] + g.yp[...]
        g.x_y.start()

    def stage4_half(g):
        g.x_y.wait_recv()
        g.yb[...] = (g.yx[...] + g.yxr[...]).astype(BF16)
        g.p_b.start()
        place(g, core * half_width, g.yb[...])

    def finish(g):
        for name in g.copies:
            g.copies[name]().wait_send()

    def stage5_half(g):
        g.p_b.wait_recv()
        place(g, (1 - core) * half_width, g.yg[...])
        finish(g)

    quarter = half_width // 2
    far_cols = pl.ds(pl.multiple_of((1 - chip) * quarter, 128), quarter)
    near_cols = pl.ds(pl.multiple_of(chip * quarter, 128), quarter)

    def stage3_quarter(g):
        g.p_y.wait_recv()
        g.yx[...] = g.ym[:, far_cols] + g.yp[:, far_cols]
        g.x_y.start()
        g.yn[...] = g.ym[:, near_cols] + g.yp[:, near_cols]

    def stage4_quarter(g):
        g.x_y.wait_recv()
        g.yb[...] = (g.yn[...] + g.yxr[...]).astype(BF16)
        g.x_b.start()
        g.p_b.start()
        place(g, core * half_width + chip * quarter, g.yb[...])

    def stage5_quarter(g):
        g.x_b.wait_recv()
        g.p_f.start()
        place(g, core * half_width + (1 - chip) * quarter, g.yg[0])

    def stage6_quarter(g):
        g.p_b.wait_recv()
        place(g, (1 - core) * half_width + chip * quarter, g.yg[1])
        g.p_f.wait_recv()
        place(g, (1 - core) * half_width + (1 - chip) * quarter, g.yg[2])
        finish(g)

    common = (stage0, stage1, stage2)
    stages = dict(half=common + (stage3_half, stage4_half, stage5_half),
                  quarter=common + (stage3_quarter, stage4_quarter, stage5_quarter, stage6_quarter))
    groups = [group(i) for i in range(len(GROUPS))]

    def attend_block(blk):
        if blk + READ_AHEAD < n_blocks:
            for c in reads(blk + READ_AHEAD):
                c.start()
        for c in reads(blk):
            c.wait()
        p = piece_of(blk)
        row = FIRST_ROWS + blk * BLOCK_ROWS
        idx = [i for i in range(len(GROUPS)) if row >= sum(GROUPS[:i])][-1]
        g = groups[idx]
        lane0 = row - g.row0
        carry = zero_carry() if lane0 == 0 else (g.ml[pl.ds(0, HEAD_PAD), :], g.ml[pl.ds(HEAD_PAD, HEAD_PAD), :])
        rows = pl.ds(blk * BLOCK_ROWS - PIECE_ROW0[p], BLOCK_ROWS)
        store_ml(g.ml, attend(row, pos_ref, base, head_dim ** -0.5, q_ref, kret[p].at[rows], vret[p].at[rows],
                              s_scr, w_scr, g.o, lane0, g.n, carry, (kn_ref, vn_ref)))

    for action in SCHEDULE:
        if isinstance(action, int):
            attend_block(action)
        elif action == 'wo':
            load_wo.wait()
        elif action == 'barrier':
            pl.semaphore_wait(barrier, 2)
        else:
            stages[KINDS[action[0]]][action[1]](groups[action[0]])


def piece_of(blk):
    return [i for i in range(N_PIECES) if blk * BLOCK_ROWS >= PIECE_ROW0[i]][-1]


BUFS = ('o', 'ml', 'pml', 'po', 'mlc', 'mlo', 'oc', 'om', 'xo', 'xml', 'ob', 'yq', 'yp', 'ym', 'yn', 'yx', 'yxr', 'yb',
        'yg')
SCHEDULE = ('barrier', (0, 0), 0, (0, 1), 1, 2, (1, 0), 3, (1, 1), 4, 5, (2, 0), 'wo', (0, 2), (2, 1), 6, (0,
            3), 7, (3, 0), (1, 2), (3, 1), (2, 2), (1, 3), (2, 3), (0, 4), (3, 2), (1, 4), (3, 3), (2, 4), (1,
            5), (1, 6), (0, 5), (3, 4), (2, 5), (3, 5), (0, 6), (2, 6))


def rest_part(pos, q, kn, vn, o0, ml0, wo, k, v):
    n_rows, seq_local, head_dim = k.shape
    rows_local, d_model = wo.shape
    units = rows_local // 128
    n_blocks = sum(PIECES) // BLOCK_ROWS

    def buffers(n, own, kind):
        span = units * n
        ml, part, half = (2 * HEAD_PAD, 128), (span, 128), (n, d_model // 2)
        slab = half if kind == 'half' else (n, d_model // 4)
        shapes = dict(o=((2 * HEAD_PAD * n if own else 8, 128), F32), ml=(ml, F32),
                      pml=(ml, F32), po=((2,) + part, F32), mlc=((16, 128), F32), mlo=((16, 128), F32), oc=(part, F32), om=(part, F32),
                      xo=(part, F32), xml=((16, 128), F32), ob=((n, rows_local), BF16), yq=(half, F32), yp=(half, F32),
                      ym=(half, F32), yn=(slab if kind != 'half' else (8, 128), F32), yx=(slab, F32),
                      yxr=(slab, F32), yb=(slab, BF16), yg=(slab if kind == 'half' else (3,) + slab, BF16))
        return [pltpu.VMEM(*shapes[name]) for name in BUFS]

    return pl.pallas_call(
        rest_kernel,
        out_shape=tuple(pltpu.VMEM((n, seq_local, head_dim), BF16) for n in PIECES * 2)
        + (pltpu.VMEM((n_rows, d_model), BF16),),
        in_specs=[SMEM_SPEC] + [VMEM_SPEC] * 5 + [ANY_SPEC] * 3,
        out_specs=(VMEM_SPEC,) * (2 * N_PIECES + 1),
        scratch_shapes=[
            pltpu.VMEM(wo.shape, BF16),
            pltpu.VMEM((BLOCK_ROWS, HEAD_PAD, seq_local), F32),
            pltpu.VMEM((BLOCK_ROWS, HEAD_PAD, seq_local), BF16),
            pltpu.VMEM((4, HEAD_PAD, 128), F32),
            DMA, DMA((n_blocks,)), DMA((n_blocks,)), DMA((len(GROUPS), COPIES)), DMA((len(GROUPS), COPIES))]
            + [b for i, n in enumerate(GROUPS) for b in buffers(n, i > 0, KINDS[i])],
        compiler_params=pltpu.CompilerParams(collective_id=0, has_side_effects=True, vmem_limit_bytes=REST_VMEM * MIB),
        cost_estimate=pl.CostEstimate(flops=10**10, bytes_accessed=40 * 10**6, transcendentals=0),
        name='attention_rest',
    )(pos, q, kn, vn, o0, ml0, wo, k, v)


REST_VMEM = 18


def write_kernel(pos_ref, kn_ref, vn_ref, y_ref, *refs):
    ko_hbm, vo_hbm, y_hbm = refs[2 * N_PIECES + 2:2 * N_PIECES + 5]
    kret, vret = refs[2 * N_PIECES + 5:3 * N_PIECES + 5], refs[3 * N_PIECES + 5:4 * N_PIECES + 5]
    k_sems, v_sems, y_sem = refs[4 * N_PIECES + 5:]
    seq_local = ko_hbm.shape[1]
    base = lax.axis_index('sp') * seq_local
    write_y = pltpu.make_async_copy(y_ref, y_hbm, y_sem)

    def writes(p):
        dst = pl.ds(FIRST_ROWS + PIECE_ROW0[p], PIECES[p])
        return (pltpu.make_async_copy(kret[p], ko_hbm.at[dst], k_sems.at[p]),
                pltpu.make_async_copy(vret[p], vo_hbm.at[dst], v_sems.at[p]))

    for p in range(N_PIECES):
        for kept, new, copy in zip((kret, vret), (kn_ref, vn_ref), writes(p)):
            patch_rows(kept[p], new, FIRST_ROWS + PIECE_ROW0[p], pos_ref, base, range(PIECES[p]))
            copy.start()
    write_y.start()
    write_y.wait()
    for p in range(N_PIECES):
        for c in writes(p):
            c.wait()


def write_part(pos, kn, vn, y, ko, vo, kret, vret):
    kept = (*kret, *vret)
    out = pl.pallas_call(
        write_kernel,
        out_shape=(jax.ShapeDtypeStruct(ko.shape, ko.dtype), jax.ShapeDtypeStruct(vo.shape, vo.dtype),
                   jax.ShapeDtypeStruct(y.shape, y.dtype)) + tuple(pltpu.VMEM(a.shape, a.dtype) for a in kept),
        in_specs=[SMEM_SPEC, VMEM_SPEC, VMEM_SPEC, VMEM_SPEC] + [VMEM_SPEC] * (2 * N_PIECES) + [ANY_SPEC, ANY_SPEC],
        out_specs=(ANY_SPEC, ANY_SPEC, ANY_SPEC) + (VMEM_SPEC,) * (2 * N_PIECES),
        input_output_aliases={4 + 2 * N_PIECES: 0, 5 + 2 * N_PIECES: 1,
                              **{4 + i: 3 + i for i in range(2 * N_PIECES)}},
        scratch_shapes=[DMA((N_PIECES,)), DMA((N_PIECES,)), DMA],
        compiler_params=pltpu.CompilerParams(vmem_limit_bytes=REST_VMEM * MIB),
        cost_estimate=pl.CostEstimate(flops=10**10, bytes_accessed=40 * 10**6, transcendentals=0),
        name='attention_write',
    )(pos, kn, vn, y, *kept, ko, vo)
    return out[2], out[0], out[1]


def in_vmem(*arrays):
    return [pltpu.with_memory_space_constraint(a, pltpu.VMEM) for a in arrays]


def solution(mesh):
    def local_step(tokens, w_query, w_key, w_value, w_out, k_cache, v_cache, positions):
        ko, vo, q, kn, vn, o0, ml0 = first_part(
            positions, tokens, w_query, w_key, w_value, k_cache, v_cache)
        q, kn, vn, o0, ml0 = in_vmem(q, kn, vn, o0, ml0)
        *kept, y = rest_part(positions, q, kn, vn, o0, ml0, w_out, k_cache, v_cache)
        *kept, y = in_vmem(*kept, y)
        return write_part(positions, kn, vn, y, ko, vo, kept[:N_PIECES], kept[N_PIECES:])

    cache_spec = P('dp', 'sp', None)
    return jax.shard_map(local_step, mesh=mesh, in_specs=(P('dp', None), P(), P(), P(), P('sp', None), cache_spec, cache_spec, P('dp')), out_specs=(P('dp', None), cache_spec, cache_spec), check_vma=False)
```
